32 devices in a mesh: pipe: 2 (over core), dp: 4 (over z), mp: 4 (over y, x).
Axes of the slice: x: 2, y: 2, z: 4, core: 2. Of those that a mesh axis runs over, the one named last changes fastest.
Arguments:
- hidden_states: bfloat16 [16, 64, 4096], P('dp'), may hold values from -6 to 6
- up_weight: bfloat16 [2, 4096, 7168], P('pipe', 'dp', 'mp'), may hold values from -0.09375 to 0.09375
- down_weight: bfloat16 [2, 7168, 4096], P('pipe', 'mp', 'dp'), may hold values from -0.0625 to 0.0625
- layer_gain: float32 [2, 4096], P('pipe'), may hold values from 0.5 to 1.5
- final_gain: float32 [4096], replicated, may hold values from 0.5 to 1.5
- unembedding: bfloat16 [32768, 4096], P(('pipe', 'mp')), may hold values from -32 to 32
- target_ids: int32 [16, 64], P('dp'), may hold values from 0 to 32767
- response_masks: int32 [16, 64], P('dp'), may hold values from 0 to 1, as said below
- anchor_logps: float32 [16, 64], P('dp'), may hold values from -14 to -10
- pairing: int32 [4, 4], P('dp'), may hold values from 0 to 3, each once within a row
Outputs:
- token_logps: float32 [16, 64], P('dp')
- seq_logps: float32 [16], P('dp')
- pair_losses: float32 [8], P('dp')
The draws below stay inside these ranges and needn't reach their ends.
Inputs may be any that keep to these rules, and one draw needn't show every extreme that they name: response_masks is 1 on one unbroken run of at least one position per sequence, starting at or after position 8, and 0 elsewhere.
All inputs are finite; a program needn't handle non-finite values.
Results may differ from the reference program's by a relative error of at most 0.0075.
Values may be sent and summed in bfloat16 or wider, within the bound.
A program may use at most 192 MiB of HBM per device.

```python
import math
import jax
import jax.numpy as jnp
import numpy as np
from jax import lax

D = 4096
VOCAB = 32768
FF = 7168
LEN = 64
SEQ_DEV = 4
SEQ_MB = 1
MICRO = 4
GROUPS = 4
SEQS = 16
PAIRS = 8
SECTIONS = 2


def draw_unembedding(key, part):
    values = jax.random.normal(key, (VOCAB, D), jnp.float32) * (2.0 * D ** (-0.5))
    values = jnp.clip(values, -12.0 * D ** (-0.5), 12.0 * D ** (-0.5))
    return values.astype(jnp.bfloat16)


def draw_response_masks(key, part):
    first_key, second_key = jax.random.split(key)
    starts = jax.random.randint(first_key, (SEQS, 1), LEN // 8, LEN // 2)
    spread = jax.random.randint(second_key, (SEQS, 1), 0, 1 << 20)
    spans = 1 + spread % (LEN - starts)
    positions = jnp.arange(LEN, dtype=jnp.int32)[None, :]
    return ((positions >= starts) & (positions < starts + spans)).astype(jnp.int32)


def set_ends(array, key, low, largest):
    spot = [jax.random.randint(jax.random.fold_in(key, axis), (), 0, length) for axis, length in enumerate(array.shape)]
    main_axis = array.shape.index(max(array.shape))
    next_to = spot[:main_axis] + [(spot[main_axis] + 1) % array.shape[main_axis]] + spot[main_axis + 1:]
    return array.at[tuple(spot)].set(low).at[tuple(next_to)].set(largest)


def steps_of(key, dims, cuts, low, largest):
    def one(axis_at, parts):
        heights = jax.random.uniform(jax.random.fold_in(jax.random.fold_in(key, 6), axis_at), (parts,), jnp.float32, low / len(cuts), largest / len(cuts))
        return jnp.repeat(jnp.exp(heights), dims[axis_at] // parts).reshape((-1,) + (1,) * (len(dims) - axis_at - 1))

    gain = one(*cuts[0])
    for cut in cuts[1:]:
        gain = gain * one(*cut)
    return gain


def rank_table(count, lean):
    portions = [(1 << 20) // math.isqrt(grade ** lean) + 1 for grade in range(1, count + 1)]
    scale = 1 + sum(portions) // (1 << 30)
    return np.cumsum(np.array([max(1, weight // scale) for weight in portions]))


def ranked_ids(rng, dims, amount, skew):
    table = rank_table(amount, skew)
    lot = jax.random.randint(jax.random.fold_in(rng, 1), dims, 0, int(table[amount - 1]))
    standing = jnp.searchsorted(jnp.asarray(table, jnp.int32), lot, side="right")
    return jax.random.permutation(jax.random.fold_in(rng, 2), amount)[standing].astype(jnp.int32)


def normal_values(own_key, dims, width, most, shards=(), kind=jnp.bfloat16):
    values = jax.random.normal(own_key, dims, jnp.float32) * width
    if len(shards) > 0:
        values = steps_of(own_key, dims, shards, -0.22, 0.18) * values
    return jnp.clip(values, min=-most, max=most).astype(kind)


def setup_inputs(seed: int = 0) -> dict:
    key_list = jax.random.split(jax.random.key(seed), 11)
    hidden_states = normal_values(key_list[0], (SEQS, LEN, D), 1.0, 6.0, ((0, 4),))
    up_weight = normal_values(key_list[1], (SECTIONS, D, FF), D ** -0.5, 0.09375, ((0, 2), (1, 4), (2, 4)))
    down_weight = normal_values(key_list[2], (SECTIONS, FF, D), FF ** -0.5, 0.0625, ((0, 2), (1, 4), (2, 4)))
    layer_gain = jnp.clip(1.0 + 0.1 * jax.random.normal(key_list[3], (SECTIONS, D), jnp.float32), 0.5, 1.5)
    final_gain = jnp.clip(1.0 + 0.1 * jax.random.normal(key_list[4], (D,), jnp.float32), 0.5, 1.5)
    unembedding = draw_unembedding(jax.random.fold_in(key_list[10], 71), 0)
    target_ids = set_ends(ranked_ids(key_list[6], (SEQS, LEN), VOCAB, 2), jax.random.fold_in(key_list[6], 3), 0, VOCAB - 1).astype(jnp.int32)
    response_masks = draw_response_masks(jax.random.fold_in(key_list[10], 71), 0)
    anchor_logps = jnp.clip(-14.0 + 4.0 * jax.random.uniform(key_list[8], (SEQS, LEN), jnp.float32) ** steps_of(key_list[8], (SEQS, LEN), ((0, 4),), -0.2, 0.2), -14.0, -10.0)
    pairing = jax.vmap(lambda own: jax.random.permutation(own, SEQ_DEV))(jax.random.split(key_list[9], GROUPS)).reshape((GROUPS, SEQ_DEV)).astype(jnp.int32)
    return dict(hidden_states=hidden_states, up_weight=up_weight, down_weight=down_weight, layer_gain=layer_gain, final_gain=final_gain, unembedding=unembedding, target_ids=target_ids, response_masks=response_masks, anchor_logps=anchor_logps, pairing=pairing)


epsilon = 1e-05
ipo_tau = 0.5

def rms_scale(values, gain_row):
    mean_square = lax.optimization_barrier(jnp.mean(values * values, axis=-1, keepdims=True))
    return values * lax.rsqrt(mean_square + epsilon) * gain_row.astype(jnp.float32)

def section_layer(states, gain_row, up_matrix, down_matrix):
    wide_states = states.astype(jnp.float32)
    normed = rms_scale(wide_states, gain_row).astype(jnp.bfloat16)
    active = jax.nn.silu(jnp.dot(normed, up_matrix, preferred_element_type=jnp.float32)).astype(jnp.bfloat16)
    summed = wide_states + jnp.dot(active, down_matrix, preferred_element_type=jnp.float32)
    return summed.astype(jnp.bfloat16)

def token_scores(finals, final_gain, unembedding, wanted_ids):
    normed = rms_scale(finals.astype(jnp.float32), final_gain).astype(jnp.bfloat16)
    logits = jnp.dot(normed, unembedding.T, preferred_element_type=jnp.float32)
    top_value = lax.optimization_barrier(jnp.max(logits, axis=1, keepdims=True))
    log_total = top_value[:, 0] + jnp.log(lax.optimization_barrier(jnp.sum(jnp.exp(logits - top_value), axis=1)))
    picked = jnp.take_along_axis(logits, wanted_ids[:, None], axis=1)[:, 0]
    return picked - log_total

def reference(hidden_states, up_weight, down_weight, layer_gain, final_gain, unembedding, target_ids, response_masks, anchor_logps, pairing):

    def one_group(group_items):
        states, wanted_ids = group_items
        flat_states = states.reshape(SEQ_DEV * LEN, D)
        for section_index in range(SECTIONS):
            flat_states = section_layer(flat_states, layer_gain[section_index], up_weight[section_index], down_weight[section_index])
        return token_scores(flat_states, final_gain, unembedding, wanted_ids.reshape(SEQ_DEV * LEN)).reshape(SEQ_DEV, LEN)
    token_logps = lax.map(one_group, (hidden_states.reshape(GROUPS, SEQ_DEV, LEN, D), target_ids.reshape(GROUPS, SEQ_DEV, LEN)))
    token_logps = token_logps.reshape(SEQS, LEN)
    mask_values = response_masks.astype(jnp.float32)
    counts = lax.optimization_barrier(jnp.sum(mask_values.reshape(GROUPS, MICRO, SEQ_MB * LEN), axis=(0, 2)))
    mean_length = counts / (GROUPS * SEQ_MB)
    divisor = jnp.tile(jnp.repeat(mean_length, SEQ_MB), GROUPS)
    policy = lax.optimization_barrier(jnp.sum(mask_values * token_logps, axis=1)) / divisor
    anchor = lax.optimization_barrier(jnp.sum(mask_values * anchor_logps, axis=1)) / divisor
    log_gaps = (policy - anchor).reshape(GROUPS, SEQ_DEV)
    chosen = jnp.take_along_axis(log_gaps, pairing[:, 0::2], axis=1)
    rejected = jnp.take_along_axis(log_gaps, pairing[:, 1::2], axis=1)
    losses = (chosen - rejected - 0.5 / ipo_tau) ** 2
    return (token_logps, policy, losses.reshape(PAIRS))
```

```python
import functools
import jax
import jax.numpy as jnp
from jax import lax
from jax.experimental import pallas as pl
from jax.experimental.pallas import tpu as pltpu
from jax.sharding import PartitionSpec as P

SEQ_MB = 1

epsilon = 1e-05
ipo_tau = 0.5
VP = ("pipe", "mp")
MESH = pl.DeviceIdType.MESH
PIECES = 8


def remote(src, dst, send_sem, recv_sem, target):
    return pltpu.make_async_remote_copy(
        src_ref=src,
        dst_ref=dst,
        send_sem=send_sem,
        recv_sem=recv_sem,
        device_id=target,
        device_id_type=MESH,
    )


def greet(axes):
    barrier = pltpu.get_barrier_semaphore()
    total = 0
    for axis in axes:
        size = lax.axis_size(axis)
        here = lax.axis_index(axis)
        for k in range(1, size):
            pl.semaphore_signal(
                barrier, inc=1, device_id={axis: lax.rem(here + k, size)}, device_id_type=MESH
            )
        total += size - 1
    pl.semaphore_wait(barrier, total)


def chunk_rows(index, size):
    return pl.ds(pl.multiple_of(index * size, 8), size)


def spread(full, size, mp_sems, pipe_sems):
    (mp_send, mp_recv), (pipe_send, pipe_recv) = mp_sems, pipe_sems
    count = lax.axis_size("mp")
    m, p = lax.axis_index("mp"), lax.axis_index("pipe")

    def to_mp(k, owner):
        rows = full.at[chunk_rows(p * count + owner, size)]
        return remote(rows, rows, mp_send.at[k], mp_recv.at[k], {"mp": lax.rem(m + k, count)})

    def to_pipe(k, pipe):
        rows = full.at[chunk_rows(pipe * count + lax.rem(m - k + count, count), size)]
        return remote(rows, rows, pipe_send.at[k], pipe_recv.at[k], {"pipe": 1 - p})

    for k in range(1, count):
        to_mp(k, m).start()
    to_pipe(0, p).start()
    for k in range(1, count):
        to_mp(k, lax.rem(m - k + count, count)).wait_recv()
        to_pipe(k, p).start()
    for k in range(count):
        to_pipe(k, 1 - p).wait_recv()
    for k in range(1, count):
        to_mp(k, m).wait_send()
    for k in range(count):
        to_pipe(k, p).wait_send()


def gather_sum(part, size, near, far, sent, sems):
    near_send, near_recv, far_send, far_recv = sems
    count = lax.axis_size("mp")
    m, p = lax.axis_index("mp"), lax.axis_index("pipe")
    order = list(range(1, count)) + [0]

    def to_core(k):
        rows = part.at[chunk_rows((1 - p) * count + lax.rem(m + k, count), size)]
        return remote(rows, near.at[k], near_send.at[k], near_recv.at[k], {"pipe": 1 - p})

    def to_chip(k):
        return remote(
            sent.at[k], far.at[k], far_send.at[k], far_recv.at[k], {"mp": lax.rem(m + k, count)}
        )

    for k in order:
        to_core(k).start()
    for k in order:
        to_core(k).wait_recv()
        own = part[chunk_rows(p * count + lax.rem(m + k, count), size), :].astype(jnp.float32)
        own = own + near[k].astype(jnp.float32)
        if k > 0:
            sent[k] = own.astype(sent.dtype)
            to_chip(k).start()
    for k in range(1, count):
        to_chip(k).wait_recv()
        own = own + far[k].astype(jnp.float32)
    for k in range(1, count):
        to_chip(k).wait_send()
    for k in order:
        to_core(k).wait_send()
    return own


def share_sum(slots, send, recv):
    count = lax.axis_size("dp")
    d = lax.axis_index("dp")

    def hop(k):
        return remote(
            slots.at[0], slots.at[k], send.at[k], recv.at[k], {"dp": lax.rem(d + k, count)}
        )

    for k in range(1, count):
        hop(k).start()
    total = slots[0]
    for k in range(1, count):
        hop(k).wait_recv()
        total = total + slots[k]
    for k in range(1, count):
        hop(k).wait_send()
    return total


def first_kernel(
    x_ref, gain_ref, blocks_ref, full_ref, normed_ref, n_send, n_recv, x_send, x_recv, ms, mr, ps, pr
):
    count = lax.axis_size("dp")
    d = lax.axis_index("dp")
    v = lax.axis_index(("pipe", "mp"))
    part, width = x_ref.shape
    block = width // count
    greet(("dp", "mp", "pipe"))
    wide = x_ref[...].astype(jnp.float32)
    scale = lax.rsqrt(jnp.mean(wide * wide, axis=-1, keepdims=True) + epsilon)
    normed_ref[...] = (wide * scale * gain_ref[...]).astype(normed_ref.dtype)

    def columns(owner):
        return pl.ds(pl.multiple_of(owner * block, 128), block)

    def normed_hop(k, owner):
        to = lax.rem(d + k, count)
        return remote(
            normed_ref.at[:, columns(to)],
            full_ref.at[chunk_rows(v * count + owner, part)],
            n_send.at[k],
            n_recv.at[k],
            {"dp": to},
        )

    def plain_hop(k, owner):
        to = lax.rem(d + k, count)
        return remote(
            x_ref.at[:, columns(to)],
            blocks_ref.at[chunk_rows(owner, part)],
            x_send.at[k],
            x_recv.at[k],
            {"dp": to},
        )

    for k in range(1, count):
        normed_hop(k, d).start()
    for k in range(1, count):
        plain_hop(k, d).start()
    full_ref[chunk_rows(v * count + d, part), :] = normed_ref[:, columns(d)]
    blocks_ref[chunk_rows(d, part), :] = x_ref[:, columns(d)]
    for k in range(1, count):
        normed_hop(k, lax.rem(d - k + count, count)).wait_recv()
    spread(full_ref, part * count, (ms, mr), (ps, pr))
    for k in range(1, count):
        plain_hop(k, lax.rem(d - k + count, count)).wait_recv()
    for k in range(1, count):
        normed_hop(k, d).wait_send()
        plain_hop(k, d).wait_send()


def middle_kernel(
    width, part_ref, resid_ref, gain_ref, blocks_ref, full_ref,
    near, far, sent, slots, ns, nr, fs, fr, qs, qr, ms, mr, ps, pr,
):
    v = lax.axis_index(("pipe", "mp"))
    size = resid_ref.shape[0]
    greet(("dp", "mp", "pipe"))
    summed = gather_sum(part_ref, size, near, far, sent, (ns, nr, fs, fr))
    value = (resid_ref[...].astype(jnp.float32) + summed).astype(jnp.bfloat16)
    blocks_ref[...] = value
    wide = value.astype(jnp.float32)
    slots[0] = lax.dot_general(
        jnp.ones((8, wide.shape[1]), jnp.float32),
        wide * wide,
        (((1,), (1,)), ((), ())),
        precision=lax.Precision.HIGHEST,
        preferred_element_type=jnp.float32,
    )
    scale = lax.rsqrt(share_sum(slots, qs, qr) / width + epsilon)
    scale = jnp.transpose(scale)[:, :1]
    wide = blocks_ref[...].astype(jnp.float32)
    full_ref[chunk_rows(v, size), :] = (wide * scale * gain_ref[...]).astype(full_ref.dtype)
    spread(full_ref, size, (ms, mr), (ps, pr))


def last_kernel(
    part_ref, resid_ref, gain_ref, full_ref,
    near, far, sent, blocks, fin, ns, nr, fs, fr, hs, hr, ms, mr, ps, pr,
):
    count = lax.axis_size("dp")
    d = lax.axis_index("dp")
    v = lax.axis_index(("pipe", "mp"))
    size, block = resid_ref.shape
    part = size // count
    greet(("dp", "mp", "pipe"))
    summed = gather_sum(part_ref, size, near, far, sent, (ns, nr, fs, fr))
    blocks[...] = (resid_ref[...].astype(jnp.float32) + summed).astype(jnp.bfloat16)

    def hop(k, owner):
        to = lax.rem(d + k, count)
        return remote(
            blocks.at[chunk_rows(to, part)], fin.at[owner], hs.at[k], hr.at[k], {"dp": to}
        )

    for k in range(1, count):
        hop(k, d).start()
    fin[d] = blocks[chunk_rows(d, part), :]
    for k in range(1, count):
        hop(k, lax.rem(d - k + count, count)).wait_recv()
    total = 0.0
    for g in range(count):
        wide = fin[g].astype(jnp.float32)
        total = total + jnp.sum(wide * wide, axis=1, keepdims=True)
    scale = lax.rsqrt(total / (block * count) + epsilon)
    for g in range(count):
        cut = slice(g * block, (g + 1) * block)
        full_ref[chunk_rows(v, part), cut] = (
            fin[g].astype(jnp.float32) * scale * gain_ref[:, cut]
        ).astype(full_ref.dtype)
    spread(full_ref, part, (ms, mr), (ps, pr))
    for k in range(1, count):
        hop(k, d).wait_send()


def stats_kernel(stats_ref, counts_ref, full_ref, total_ref, slots, qs, qr, ms, mr, ps, pr):
    v = lax.axis_index(("pipe", "mp"))
    size = stats_ref.shape[0]
    greet(("dp", "mp", "pipe"))
    slots[0] = counts_ref[...]
    full_ref[chunk_rows(v, size), :] = stats_ref[...]
    total_ref[...] = share_sum(slots, qs, qr)
    spread(full_ref, size, (ms, mr), (ps, pr))


def chain_kernel(h_ref, out_ref, arrived, summed, rs, rr, gs, gr):
    count = lax.axis_size("dp")
    d = lax.axis_index("dp")
    half = h_ref.shape[0] // 2
    rows = half // PIECES
    right, left = lax.rem(d + 1, count), lax.rem(d + count - 1, count)
    barrier = pltpu.get_barrier_semaphore()
    for has, who in ((d > 0, left), (d < count - 1, right)):

        @pl.when(has)
        def _():
            pl.semaphore_signal(barrier, inc=1, device_id={"dp": who}, device_id_type=MESH)

    ends = (d > 0).astype(jnp.int32) + (d < count - 1).astype(jnp.int32)
    pl.semaphore_wait(barrier, ends)

    hops = (d, count - 1 - d)

    def cut(way, c):
        return pl.ds(pl.multiple_of((1 - way) * half + c * rows, 16), rows)

    def onward_copy(way, c, source):
        to = (right, left)[way]
        return remote(source, arrived.at[way, c], rs.at[way, c], rr.at[way, c], {"dp": to})

    def back_copy(way, c):
        spot = out_ref.at[cut(way, c)]
        to = (left, right)[way]
        return remote(spot, spot, gs.at[way, c], gr.at[way, c], {"dp": to})

    for way in range(2):

        @pl.when(hops[way] == 0)
        def _():
            for c in range(PIECES):
                onward_copy(way, c, h_ref.at[cut(way, c)]).start()

    def step(t, carry):
        for way in range(2):
            before = hops[way]
            c = t - before

            @pl.when((before > 0) & (c >= 0) & (c < PIECES))
            def _():
                onward_copy(way, c, summed.at[way, c]).wait_recv()
                total = arrived[way, c].astype(jnp.float32) + h_ref[cut(way, c), :].astype(jnp.float32)

                @pl.when(before < count - 1)
                def _():
                    summed[way, c] = total.astype(summed.dtype)
                    onward_copy(way, c, summed.at[way, c]).start()

                @pl.when(before == count - 1)
                def _():
                    out_ref[cut(way, c), :] = (total / (1.0 + jnp.exp(-total))).astype(
                        out_ref.dtype
                    )
                    back_copy(way, c).start()

        for way in range(2):
            after = count - 1 - hops[way]
            g = t - (count - 1) - after

            @pl.when((after > 0) & (g >= 0) & (g < PIECES))
            def _():
                back_copy(way, g).wait_recv()

                @pl.when(after < count - 1)
                def _():
                    back_copy(way, g).start()

        return carry

    lax.fori_loop(0, PIECES + 2 * (count - 1), step, 0)
    for way in range(2):

        @pl.when(hops[way] < count - 1)
        def _():
            for c in range(PIECES):
                onward_copy(way, c, summed.at[way, c]).wait_send()

        @pl.when(hops[way] > 0)
        def _():
            for c in range(PIECES):
                back_copy(way, c).wait_send()


def call(kernel, name, ident, outs, scratch, *args):
    spec = pl.BlockSpec(memory_space=pltpu.VMEM)
    return pl.pallas_call(
        kernel,
        name=name,
        out_shape=outs,
        in_specs=[spec] * len(args),
        out_specs=jax.tree.map(lambda _: spec, outs),
        scratch_shapes=scratch,
        compiler_params=pltpu.CompilerParams(collective_id=ident, has_side_effects=True),
    )(*args)


def sems(*shape):
    return [pltpu.SemaphoreType.DMA(shape)] * 2


def shards(
    hidden_states,
    up_weight,
    down_weight,
    layer_gain,
    final_gain,
    unembedding,
    target_ids,
    response_masks,
    anchor_logps,
    pairing,
):
    seq_count, length, model_width = hidden_states.shape
    groups = lax.axis_size("dp")
    vp_size = lax.axis_size("pipe") * lax.axis_size("mp")
    vp_index = lax.axis_index(VP)
    dp_index = lax.axis_index("dp")
    pipe_index = lax.axis_index("pipe")
    rows = seq_count * length
    part = rows // vp_size
    block = model_width // groups
    mask_values = response_masks.astype(jnp.float32)
    local_counts = jnp.sum(mask_values, axis=1)
    count = lax.axis_size("mp")
    bf16 = jnp.bfloat16
    spread_sems = sems(count) + sems(count)
    reach_sems = sems(count) + sems(count)
    buffers = [pltpu.VMEM((count, part, block), bf16) for part in [rows // vp_size * groups]] * 3

    up_own, down_own = up_weight[0], down_weight[0]
    half = up_own.shape[1] // 2
    away = (1 - pipe_index) * half
    keep = pipe_index * half
    swap = [(0, 1), (1, 0)]
    gain_other = lax.ppermute(layer_gain, "pipe", swap)
    up_other = lax.ppermute(lax.dynamic_slice_in_dim(up_own, away, half, 1), "pipe", swap)
    down_other = lax.ppermute(lax.dynamic_slice_in_dim(down_own, away, half, 0), "pipe", swap)
    up_mine = lax.dynamic_slice_in_dim(up_own, keep, half, 1)
    down_mine = lax.dynamic_slice_in_dim(down_own, keep, half, 0)

    def section_of(s):
        own = pipe_index == s
        gain = jnp.where(own, layer_gain[0], gain_other[0])
        return (
            lax.dynamic_slice_in_dim(gain, dp_index * block, block, 0),
            jnp.where(own, up_mine, up_other),
            jnp.where(own, down_mine, down_other),
        )

    mine = lax.dynamic_slice_in_dim(
        hidden_states.reshape(rows, model_width), vp_index * part, part, 0
    )
    size = part * groups
    total_rows = rows * groups
    blocks, full = call(
        first_kernel,
        "first",
        0,
        [
            jax.ShapeDtypeStruct((size, block), bf16),
            jax.ShapeDtypeStruct((total_rows, block), bf16),
        ],
        [pltpu.VMEM((part, model_width), bf16)] + sems(groups) + sems(groups) + spread_sems,
        mine,
        jnp.where(pipe_index == 0, layer_gain, gain_other),
    )
    for s in range(2):
        gain, up, down = section_of(s)
        hidden = jnp.dot(full, up, preferred_element_type=jnp.float32).astype(bf16)
        piece = hidden.shape[0] // (2 * PIECES)
        active = call(
            chain_kernel,
            "chain",
            1,
            jax.ShapeDtypeStruct(hidden.shape, bf16),
            [pltpu.VMEM((2, PIECES, piece, half), bf16)] * 2 + sems(2, PIECES) + sems(2, PIECES),
            hidden,
        )
        out = jnp.dot(active, down, preferred_element_type=jnp.float32).astype(bf16)
        if s == 0:
            gain = section_of(1)[0]
            blocks, full = call(
                functools.partial(middle_kernel, model_width),
                "middle",
                2,
                [
                    jax.ShapeDtypeStruct((size, block), bf16),
                    jax.ShapeDtypeStruct((total_rows, block), bf16),
                ],
                buffers
                + [pltpu.VMEM((groups, 8, size), jnp.float32)]
                + reach_sems
                + sems(groups)
                + spread_sems,
                out,
                blocks,
                gain[None],
            )
        else:
            normed_final = call(
                last_kernel,
                "last",
                3,
                jax.ShapeDtypeStruct((rows, model_width), bf16),
                buffers
                + [pltpu.VMEM((size, block), bf16), pltpu.VMEM((groups, part, block), bf16)]
                + reach_sems
                + sems(groups)
                + spread_sems,
                out,
                blocks,
                final_gain[None],
            )
    logits = lax.dot_general(
        normed_final, unembedding, (((1,), (1,)), ((), ())), preferred_element_type=jnp.float32
    )
    vocab_start = vp_index * unembedding.shape[0]
    local_ids = target_ids.reshape(-1) - vocab_start
    columns = lax.broadcasted_iota(jnp.int32, logits.shape, 1)
    picked = jnp.sum(jnp.where(columns == local_ids[:, None], logits, 0.0), axis=1)
    local_top = jnp.max(logits, axis=1)
    local_sum = jnp.sum(jnp.exp(logits - local_top[:, None]), axis=1)
    stats = jnp.pad(jnp.stack([local_top, local_sum, picked]), ((0, 5), (0, 0)))
    padded = jnp.pad(local_counts[None], ((0, 7), (0, -seq_count % 128)))
    stats, counts = call(
        stats_kernel,
        "stats",
        4,
        [
            jax.ShapeDtypeStruct((vp_size * 8, rows), jnp.float32),
            jax.ShapeDtypeStruct(padded.shape, jnp.float32),
        ],
        [pltpu.VMEM((groups,) + padded.shape, jnp.float32)] + sems(groups) + spread_sems,
        stats,
        padded,
    )
    stats = stats.reshape(vp_size, 8, rows)
    counts = counts[0, :seq_count]
    top_value = jnp.max(stats[:, 0], axis=0)
    exp_total = jnp.sum(stats[:, 1] * jnp.exp(stats[:, 0] - top_value), axis=0)
    picked_all = jnp.sum(stats[:, 2], axis=0)
    token_logps = (picked_all - top_value - jnp.log(exp_total)).reshape(seq_count, length)

    divisor = jnp.repeat(counts / (groups * SEQ_MB), SEQ_MB)
    policy = jnp.sum(mask_values * token_logps, axis=1) / divisor
    anchor = jnp.sum(mask_values * anchor_logps, axis=1) / divisor
    log_gaps = policy - anchor
    positions = jnp.arange(seq_count, dtype=jnp.int32)
    chosen = jnp.sum(
        jnp.where(pairing[0, 0::2][:, None] == positions[None, :], log_gaps[None, :], 0.0), axis=1
    )
    rejected = jnp.sum(
        jnp.where(pairing[0, 1::2][:, None] == positions[None, :], log_gaps[None, :], 0.0), axis=1
    )
    losses = (chosen - rejected - 0.5 / ipo_tau) ** 2
    return (token_logps, policy, losses)


def solution(mesh):
    return jax.shard_map(
        shards,
        mesh=mesh,
        in_specs=(
            P("dp", None, None),
            P("pipe", "dp", "mp"),
            P("pipe", "mp", "dp"),
            P("pipe", None),
            P(),
            P(("pipe", "mp"), None),
            P("dp", None),
            P("dp", None),
            P("dp", None),
            P("dp", None),
        ),
        out_specs=(P("dp", None), P("dp"), P("dp")),
        check_vma=False,
    )
```

```python
import functools
import jax
import jax.numpy as jnp
from jax import lax
from jax.experimental import pallas as pl
from jax.experimental.pallas import tpu as pltpu
from jax.sharding import PartitionSpec as P

SEQ_MB = 1

epsilon = 1e-05
ipo_tau = 0.5
VP = ("pipe", "mp")
MESH = pl.DeviceIdType.MESH
BATCHES = 4
PIECES = 4
HOP = 2
STEP = 2


def remote(src, dst, send_sem, recv_sem, target):
    return pltpu.make_async_remote_copy(
        src_ref=src,
        dst_ref=dst,
        send_sem=send_sem,
        recv_sem=recv_sem,
        device_id=target,
        device_id_type=MESH,
    )


def greet(axes):
    barrier = pltpu.get_barrier_semaphore()
    total = 0
    for axis in axes:
        size = lax.axis_size(axis)
        here = lax.axis_index(axis)
        for k in range(1, size):
            pl.semaphore_signal(
                barrier, inc=1, device_id={axis: lax.rem(here + k, size)}, device_id_type=MESH
            )
        total += size - 1
    pl.semaphore_wait(barrier, total)


def chunk_rows(index, size):
    return pl.ds(pl.multiple_of(index * size, 8), size)


def spread(full, size, mp_sems, pipe_sems):
    (mp_send, mp_recv), (pipe_send, pipe_recv) = mp_sems, pipe_sems
    count = lax.axis_size("mp")
    m, p = lax.axis_index("mp"), lax.axis_index("pipe")

    def to_mp(k, owner):
        rows = full.at[chunk_rows(p * count + owner, size)]
        return remote(rows, rows, mp_send.at[k], mp_recv.at[k], {"mp": lax.rem(m + k, count)})

    def to_pipe(k, pipe):
        rows = full.at[chunk_rows(pipe * count + lax.rem(m - k + count, count), size)]
        return remote(rows, rows, pipe_send.at[k], pipe_recv.at[k], {"pipe": 1 - p})

    for k in range(1, count):
        to_mp(k, m).start()
    to_pipe(0, p).start()
    for k in range(1, count):
        to_mp(k, lax.rem(m - k + count, count)).wait_recv()
        to_pipe(k, p).start()
    for k in range(count):
        to_pipe(k, 1 - p).wait_recv()
    for k in range(1, count):
        to_mp(k, m).wait_send()
    for k in range(count):
        to_pipe(k, p).wait_send()


def share_sum(slots, send, recv):
    count = lax.axis_size("dp")
    d = lax.axis_index("dp")

    def hop(k):
        return remote(
            slots.at[0], slots.at[k], send.at[k], recv.at[k], {"dp": lax.rem(d + k, count)}
        )

    for k in range(1, count):
        hop(k).start()
    total = slots[0]
    for k in range(1, count):
        hop(k).wait_recv()
        total = total + slots[k]
    for k in range(1, count):
        hop(k).wait_send()
    return total


def stats_kernel(stats_ref, counts_ref, full_ref, total_ref, slots, qs, qr, ms, mr, ps, pr):
    v = lax.axis_index(("pipe", "mp"))
    size = stats_ref.shape[0]
    greet(("dp", "mp", "pipe"))
    slots[0] = counts_ref[...]
    full_ref[chunk_rows(v, size), :] = stats_ref[...]
    total_ref[...] = share_sum(slots, qs, qr)
    spread(full_ref, size, (ms, mr), (ps, pr))


def meet():
    barrier = pltpu.get_barrier_semaphore()
    n, count = lax.axis_size("dp"), lax.axis_size("mp")
    d, m, p = lax.axis_index("dp"), lax.axis_index("mp"), lax.axis_index("pipe")
    for k in range(1, n):
        pl.semaphore_signal(
            barrier, inc=1, device_id={"dp": lax.rem(d + k, n)}, device_id_type=MESH
        )
    for k in range(1, count):
        pl.semaphore_signal(
            barrier, inc=1, device_id={"mp": lax.rem(m + k, count)}, device_id_type=MESH
        )
    for k in range(count):
        pl.semaphore_signal(
            barrier,
            inc=1,
            device_id={"mp": lax.rem(m + k, count), "pipe": 1 - p},
            device_id_type=MESH,
        )
    pl.semaphore_wait(barrier, n - 1 + count - 1 + count)


def relay_kernel(
    x_hbm, up_hbm, down_hbm, layer_gain, final_gain, full_ref,
    up, down, xs, normed, xin, hid, act, ext, outs, rs, resid, nxt, slots, fin,
    load, go, ns, nr, xs_s, xs_r, gs, gr, ins, inr, exr, bs, br, rss, rsr, ds, dr, qs, qr,
    hs, hr, fs, fr, es, er,
):
    n, count = lax.axis_size("dp"), lax.axis_size("mp")
    d, m, p = lax.axis_index("dp"), lax.axis_index("mp"), lax.axis_index("pipe")
    length, width = x_hbm.shape
    block, ff = up.shape
    part = length // count
    sub = part // BATCHES
    own_rows = sub * n
    batch = own_rows * count
    half = batch // 2
    piece = half // PIECES
    total = BATCHES * PIECES
    f32 = jnp.float32

    def rows(start, size):
        return pl.ds(pl.multiple_of(start, 16), size)

    def columns(owner):
        return pl.ds(pl.multiple_of(owner * block, 128), block)

    loads = [
        pltpu.make_async_copy(x_hbm.at[rows(m * part, part)], xs, load.at[0]),
        pltpu.make_async_copy(up_hbm, up, load.at[1]),
        pltpu.make_async_copy(down_hbm, down, load.at[2]),
    ]
    for copy in loads:
        copy.start()
    meet()
    loads[0].wait()

    def first_hop(b, k, owner):
        to = lax.rem(d + k, n)
        return remote(
            normed.at[rows(b * sub, sub), columns(to)],
            xin.at[rows(b * batch + (m * n + owner) * sub, sub)],
            ns.at[b, k],
            nr.at[b, k],
            {"dp": to},
        )

    def plain_hop(b, k, owner):
        to = lax.rem(d + k, n)
        return remote(
            xs.at[rows(b * sub, sub), columns(to)],
            resid.at[rows(b * own_rows + owner * sub, sub)],
            xs_s.at[b, k],
            xs_r.at[b, k],
            {"dp": to},
        )

    def share(b, k, owner):
        slab = xin.at[rows(b * batch + owner * own_rows, own_rows)]
        return remote(slab, slab, gs.at[b, k], gr.at[b, k], {"mp": lax.rem(m + k, count)})

    def scatter(b, k):
        to = lax.rem(m + k, count)
        return remote(
            outs.at[rows(b * batch + to * own_rows, own_rows)],
            rs.at[rows((b * count + k) * own_rows, own_rows)],
            rss.at[b, k],
            rsr.at[b, k],
            {"mp": to, "pipe": 1 - p},
        )

    def hand_over(b):
        slab = rows(b * own_rows, own_rows)
        return remote(nxt.at[slab], resid.at[slab], ds.at[b], dr.at[b], {"pipe": 1 - p})

    def square(b, k):
        return remote(
            slots.at[b, 0], slots.at[b, k], qs.at[b, k], qr.at[b, k], {"dp": lax.rem(d + k, n)}
        )

    def last_hop(b, k, owner):
        to = lax.rem(d + k, n)
        return remote(
            nxt.at[rows(b * own_rows + to * sub, sub)],
            fin.at[b, owner],
            hs.at[b, k],
            hr.at[b, k],
            {"dp": to},
        )

    def spot(b, owner):
        return full_ref.at[rows(owner * part + b * sub, sub)]

    def full_share(b, k, owner):
        return remote(
            spot(b, owner), spot(b, owner), fs.at[b, k], fr.at[b, k], {"mp": lax.rem(m + k, count)}
        )

    def full_pass(b, k):
        owner = lax.rem(m - k + count, count)
        return remote(
            spot(b, owner), spot(b, owner), es.at[b, k], er.at[b, k], {"pipe": 1 - p}
        )

    def before(k):
        return lax.rem(d - k + n, n)

    def beside(k):
        return lax.rem(m - k + count, count)

    @pl.when(p == 0)
    def _():
        wide = xs[...].astype(f32)
        scale = lax.rsqrt(jnp.mean(wide * wide, axis=-1, keepdims=True) + epsilon)
        normed[...] = (wide * scale * layer_gain[...]).astype(normed.dtype)
        for b in range(BATCHES):
            for k in range(1, n):
                first_hop(b, k, d).start()
        for b in range(BATCHES):
            xin[rows(b * batch + (m * n + d) * sub, sub), :] = normed[
                b * sub : (b + 1) * sub, columns(d)
            ]
        for b in range(BATCHES):
            for k in range(1, n):
                first_hop(b, k, before(k)).wait_recv()
            for k in range(1, count):
                share(b, k, m).start()
        pl.semaphore_signal(go, inc=1, device_id={"pipe": 1 - p}, device_id_type=MESH)

    @pl.when(p == 1)
    def _():
        pl.semaphore_wait(go, 1)
        for b in range(BATCHES):
            for k in range(1, n):
                plain_hop(b, k, d).start()
            resid[rows(b * own_rows + d * sub, sub), :] = xs[b * sub : (b + 1) * sub, columns(d)]

    loads[1].wait()
    loads[2].wait()

    def enter(b):
        for k in range(1, count):
            share(b, k, beside(k)).wait_recv()
        where = rows(b * batch, batch)
        states = xin[where, :]
        step = 256
        for j in range(0, ff, step):
            hid[where, j : j + step] = jnp.dot(
                states, up[:, j : j + step], preferred_element_type=f32
            ).astype(hid.dtype)

    def leave(b):
        where = rows(b * batch, batch)
        states = act[where, :]
        step = min(block, 256)
        for j in range(0, block, step):
            outs[where, j : j + step] = jnp.dot(
                states, down[:, j : j + step], preferred_element_type=f32
            ).astype(outs.dtype)
        for k in (*range(1, count), 0):
            scatter(b, k).start()

    def add_up(b):
        for k in range(count):
            scatter(b, k).wait_recv()
        slab = rows(b * own_rows, own_rows)
        value = resid[slab, :].astype(f32)
        for k in range(count):
            value = value + rs[rows((b * count + k) * own_rows, own_rows), :].astype(f32)
        value = value.astype(nxt.dtype)
        nxt[slab, :] = value
        return value.astype(f32)

    def settle(b):
        for k in range(1, n):
            plain_hop(b, k, before(k)).wait_recv()
        wide = add_up(b)
        sums = jnp.sum(wide * wide, axis=1, keepdims=True)
        slots[b, 0] = jnp.broadcast_to(sums, (own_rows, 128))
        for k in range(1, n):
            square(b, k).start()
        hand_over(b).start()

    def renew(b):
        sums = slots[b, 0]
        for k in range(1, n):
            square(b, k).wait_recv()
            sums = sums + slots[b, k]
        scale = lax.rsqrt(sums[:, :1] / width + epsilon)
        wide = nxt[rows(b * own_rows, own_rows), :].astype(f32)
        gain = layer_gain[:, columns(d)]
        xin[rows(b * batch + m * own_rows, own_rows), :] = (wide * scale * gain).astype(xin.dtype)
        for k in range(1, count):
            share(b, k, m).start()

    def span(way, c):
        b, k = lax.div(c, PIECES), lax.rem(c, PIECES)
        return rows(b * batch + way * half + k * piece, piece)

    def inner(way, c, to, into, sem):
        return remote(hid.at[span(way, c)], into, ins.at[way, c], sem.at[way, c], {"dp": to})

    def to_act(way, c, to):
        return inner(way, c, to, act.at[span(way, c)], inr)

    def to_ext(way, c, to):
        return inner(way, c, to, ext.at[rows(c * piece, piece)], exr)

    def outer(way, c, side):
        where = act.at[span(way, c)]
        to = d - 1 if side == 0 else d + 1
        return remote(where, where, bs.at[way, c, side], br.at[way, c], {"dp": to})

    offset = 2 * STEP + 1
    deep = HOP * (n // 2)
    ticks = offset + total + 2 * deep

    def tick(t, carry):
        now = t - offset
        for way in range(2):
            owner = n // 2 - way
            left, right = d < owner, d > owner
            hops = jnp.where(left, d, n - 1 - d)
            c = now - HOP * hops

            @pl.when((d != owner) & (c >= 0) & (c < total))
            def _():
                here = span(way, c)

                @pl.when(hops > 0)
                def _():
                    to_act(way, c, d).wait_recv()
                    for j in range(0, ff, 256):
                        cut = slice(j, j + 256)
                        hid[here, cut] = (
                            hid[here, cut].astype(f32) + act[here, cut].astype(f32)
                        ).astype(hid.dtype)

                @pl.when(left)
                def _():
                    to_act(way, c, d + 1).start()

                @pl.when(right & (d - 1 > owner))
                def _():
                    to_act(way, c, d - 1).start()

                @pl.when(right & (d - 1 == owner))
                def _():
                    to_ext(way, c, d - 1).start()

        for way in range(2):
            owner = n // 2 - way
            c = now - deep

            @pl.when((d == owner) & (c >= 0) & (c < total))
            def _():
                here = span(way, c)
                there = rows(c * piece, piece)
                if owner > 0:
                    to_act(way, c, d).wait_recv()
                if owner < n - 1:
                    to_ext(way, c, d).wait_recv()
                for j in range(0, ff, 256):
                    cut = slice(j, j + 256)
                    value = hid[here, cut].astype(f32)
                    if owner > 0:
                        value = value + act[here, cut].astype(f32)
                    if owner < n - 1:
                        value = value + ext[there, cut].astype(f32)
                    act[here, cut] = (value / (1.0 + jnp.exp(-value))).astype(act.dtype)
                if owner > 0:
                    outer(way, c, 0).start()
                if owner < n - 1:
                    outer(way, c, 1).start()

        for way in range(2):
            owner = n // 2 - way
            left, right = d < owner, d > owner
            away = jnp.where(left, owner - d, d - owner)
            c = now - deep - HOP * away

            @pl.when((d != owner) & (c >= 0) & (c < total))
            def _():
                outer(way, c, 0).wait_recv()

                @pl.when(left & (d > 0))
                def _():
                    outer(way, c, 0).start()

                @pl.when(right & (d < n - 1))
                def _():
                    outer(way, c, 1).start()

        b = lax.div(now + 1, PIECES)

        @pl.when((now + 1 >= 0) & (lax.rem(now + 1, PIECES) == 0) & (b < BATCHES))
        def _():
            enter(b)

        done = now - (PIECES - 1) - 2 * deep
        q = lax.div(done, PIECES)

        @pl.when((done >= 0) & (lax.rem(done, PIECES) == 0) & (q < BATCHES))
        def _():
            leave(q)

        late = now + 1 + STEP
        e = lax.div(late, PIECES)

        @pl.when((p == 1) & (late >= 0) & (lax.rem(late, PIECES) == 0) & (e < BATCHES))
        def _():
            renew(e)

        early = now + 1 + 2 * STEP
        a = lax.div(early, PIECES)

        @pl.when((p == 1) & (lax.rem(early, PIECES) == 0) & (a < BATCHES))
        def _():
            settle(a)

        return carry

    lax.fori_loop(0, ticks, tick, 0)

    @pl.when(p == 0)
    def _():
        def finish(b, carry):
            hand_over(b).wait_recv()
            add_up(b)
            for k in range(1, n):
                last_hop(b, k, d).start()
            fin[b, d] = nxt[rows(b * own_rows + d * sub, sub), :]
            for k in range(1, n):
                last_hop(b, k, before(k)).wait_recv()
            sums = 0.0
            for g in range(n):
                wide = fin[b, g].astype(f32)
                sums = sums + jnp.sum(wide * wide, axis=1, keepdims=True)
            scale = lax.rsqrt(sums / width + epsilon)
            for g in range(n):
                cut = slice(g * block, (g + 1) * block)
                full_ref[rows(m * part + b * sub, sub), cut] = (
                    fin[b, g].astype(f32) * scale * final_gain[:, cut]
                ).astype(full_ref.dtype)
            for k in range(1, count):
                full_share(b, k, m).start()
            full_pass(b, 0).start()
            for k in range(1, count):
                full_share(b, k, beside(k)).wait_recv()
                full_pass(b, k).start()
            return carry

        lax.fori_loop(0, BATCHES, finish, 0)

    @pl.when(p == 1)
    def _():
        def finish(b, carry):
            for k in range(count):
                full_pass(b, k).wait_recv()
            return carry

        lax.fori_loop(0, BATCHES, finish, 0)

    def drain(b, carry):
        for k in range(1, count):
            share(b, k, m).wait_send()
        for k in range(count):
            scatter(b, k).wait_send()

        @pl.when(p == 0)
        def _():
            for k in range(1, n):
                first_hop(b, k, d).wait_send()
                last_hop(b, k, d).wait_send()
            for k in range(1, count):
                full_share(b, k, m).wait_send()
            for k in range(count):
                full_pass(b, k).wait_send()

        @pl.when(p == 1)
        def _():
            for k in range(1, n):
                plain_hop(b, k, d).wait_send()
                square(b, k).wait_send()
            hand_over(b).wait_send()

        return carry

    lax.fori_loop(0, BATCHES, drain, 0)

    def drain_pieces(c, carry):
        for way in range(2):
            owner = n // 2 - way

            @pl.when(d != owner)
            def _():
                to_act(way, c, d).wait_send()

            @pl.when((d <= owner) & (d > 0))
            def _():
                outer(way, c, 0).wait_send()

            @pl.when((d >= owner) & (d < n - 1))
            def _():
                outer(way, c, 1).wait_send()

        return carry

    lax.fori_loop(0, total, drain_pieces, 0)


def call(kernel, name, ident, outs, scratch, *args):
    spec = pl.BlockSpec(memory_space=pltpu.VMEM)
    return pl.pallas_call(
        kernel,
        name=name,
        out_shape=outs,
        in_specs=[spec] * len(args),
        out_specs=jax.tree.map(lambda _: spec, outs),
        scratch_shapes=scratch,
        compiler_params=pltpu.CompilerParams(collective_id=ident, has_side_effects=True),
    )(*args)


def sems(*shape):
    return [pltpu.SemaphoreType.DMA(shape)] * 2


def shards(
    hidden_states,
    up_weight,
    down_weight,
    layer_gain,
    final_gain,
    unembedding,
    target_ids,
    response_masks,
    anchor_logps,
    pairing,
):
    seq_count, length, model_width = hidden_states.shape
    groups = lax.axis_size("dp")
    vp_size = lax.axis_size("pipe") * lax.axis_size("mp")
    vp_index = lax.axis_index(VP)
    rows = seq_count * length
    block = model_width // groups
    ff = up_weight.shape[2]
    mask_values = response_masks.astype(jnp.float32)
    local_counts = jnp.sum(mask_values, axis=1)
    count = lax.axis_size("mp")
    bf16 = jnp.bfloat16
    spread_sems = sems(count) + sems(count)
    part = rows // count
    own_rows = part * groups
    all_rows = rows * groups
    steps = BATCHES * PIECES
    anyspec = pl.BlockSpec(memory_space=pl.ANY)
    spec = pl.BlockSpec(memory_space=pltpu.VMEM)
    dma = pltpu.SemaphoreType.DMA
    normed_final = pl.pallas_call(
        relay_kernel,
        name="relay",
        out_shape=jax.ShapeDtypeStruct((rows, model_width), bf16),
        in_specs=[anyspec, anyspec, anyspec, spec, spec],
        out_specs=spec,
        scratch_shapes=[
            pltpu.VMEM((block, ff), bf16),
            pltpu.VMEM((ff, block), bf16),
            pltpu.VMEM((part, model_width), bf16),
            pltpu.VMEM((part, model_width), bf16),
            pltpu.VMEM((all_rows, block), bf16),
            pltpu.VMEM((all_rows, ff), bf16),
            pltpu.VMEM((all_rows, ff), bf16),
            pltpu.VMEM((all_rows // 2, ff), bf16),
            pltpu.VMEM((all_rows, block), bf16),
            pltpu.VMEM((all_rows, block), bf16),
            pltpu.VMEM((own_rows, block), bf16),
            pltpu.VMEM((own_rows, block), bf16),
            pltpu.VMEM((BATCHES, groups, own_rows // BATCHES, 128), jnp.float32),
            pltpu.VMEM((BATCHES, groups, part // BATCHES, block), bf16),
            dma((3,)),
            pltpu.SemaphoreType.REGULAR,
        ]
        + sems(BATCHES, groups)
        + sems(BATCHES, groups)
        + sems(BATCHES, count)
        + [dma((2, steps))] * 3
        + [dma((2, steps, 2)), dma((2, steps))]
        + sems(BATCHES, count)
        + sems(BATCHES)
        + sems(BATCHES, groups)
        + sems(BATCHES, groups)
        + sems(BATCHES, count)
        + sems(BATCHES, count),
        compiler_params=pltpu.CompilerParams(
            collective_id=0, has_side_effects=True, vmem_limit_bytes=62 * 1024 * 1024
        ),
    )(
        hidden_states.reshape(rows, model_width),
        up_weight[0],
        down_weight[0],
        layer_gain,
        final_gain[None],
    )
    logits = lax.dot_general(
        normed_final, unembedding, (((1,), (1,)), ((), ())), preferred_element_type=jnp.float32
    )
    vocab_start = vp_index * unembedding.shape[0]
    local_ids = target_ids.reshape(-1) - vocab_start
    columns = lax.broadcasted_iota(jnp.int32, logits.shape, 1)
    picked = jnp.sum(jnp.where(columns == local_ids[:, None], logits, 0.0), axis=1)
    local_top = jnp.max(logits, axis=1)
    local_sum = jnp.sum(jnp.exp(logits - local_top[:, None]), axis=1)
    stats = jnp.pad(jnp.stack([local_top, local_sum, picked]), ((0, 5), (0, 0)))
    padded = jnp.pad(local_counts[None], ((0, 7), (0, -seq_count % 128)))
    stats, counts = call(
        stats_kernel,
        "stats",
        1,
        [
            jax.ShapeDtypeStruct((vp_size * 8, rows), jnp.float32),
            jax.ShapeDtypeStruct(padded.shape, jnp.float32),
        ],
        [pltpu.VMEM((groups,) + padded.shape, jnp.float32)] + sems(groups) + spread_sems,
        stats,
        padded,
    )
    stats = stats.reshape(vp_size, 8, rows)
    counts = counts[0, :seq_count]
    top_value = jnp.max(stats[:, 0], axis=0)
    exp_total = jnp.sum(stats[:, 1] * jnp.exp(stats[:, 0] - top_value), axis=0)
    picked_all = jnp.sum(stats[:, 2], axis=0)
    token_logps = (picked_all - top_value - jnp.log(exp_total)).reshape(seq_count, length)

    divisor = jnp.repeat(counts / (groups * SEQ_MB), SEQ_MB)
    policy = jnp.sum(mask_values * token_logps, axis=1) / divisor
    anchor = jnp.sum(mask_values * anchor_logps, axis=1) / divisor
    log_gaps = policy - anchor
    positions = jnp.arange(seq_count, dtype=jnp.int32)
    chosen = jnp.sum(
        jnp.where(pairing[0, 0::2][:, None] == positions[None, :], log_gaps[None, :], 0.0), axis=1
    )
    rejected = jnp.sum(
        jnp.where(pairing[0, 1::2][:, None] == positions[None, :], log_gaps[None, :], 0.0), axis=1
    )
    losses = (chosen - rejected - 0.5 / ipo_tau) ** 2
    return (token_logps, policy, losses)


def solution(mesh):
    return jax.shard_map(
        shards,
        mesh=mesh,
        in_specs=(
            P("dp", None, None),
            P("pipe", "dp", "mp"),
            P("pipe", "mp", "dp"),
            P("pipe", None),
            P(),
            P(("pipe", "mp"), None),
            P("dp", None),
            P("dp", None),
            P("dp", None),
            P("dp", None),
        ),
        out_specs=(P("dp", None), P("dp"), P("dp")),
        check_vma=False,
    )
```

```python
import math
import jax
import jax.numpy as jnp
from jax import lax
from jax.experimental import pallas as pl
from jax.experimental.pallas import tpu as pltpu
from jax.sharding import PartitionSpec as P

SEQ_MB = 1

epsilon = 1e-05
ipo_tau = 0.5
MESH = pl.DeviceIdType.MESH
BATCHES = 4
PIECES = 4
HOP = 2
STEP = 2
ROOM = 62 * 1024 * 1024


def remote(src, dst, send_sem, recv_sem, target):
    return pltpu.make_async_remote_copy(
        src_ref=src,
        dst_ref=dst,
        send_sem=send_sem,
        recv_sem=recv_sem,
        device_id=target,
        device_id_type=MESH,
    )


def meet():
    barrier = pltpu.get_barrier_semaphore()
    n, count = lax.axis_size("dp"), lax.axis_size("mp")
    d, m, p = lax.axis_index("dp"), lax.axis_index("mp"), lax.axis_index("pipe")
    for k in range(1, n):
        pl.semaphore_signal(
            barrier, inc=1, device_id={"dp": lax.rem(d + k, n)}, device_id_type=MESH
        )
    for k in range(1, count):
        pl.semaphore_signal(
            barrier, inc=1, device_id={"mp": lax.rem(m + k, count)}, device_id_type=MESH
        )
    for k in range(count):
        pl.semaphore_signal(
            barrier,
            inc=1,
            device_id={"mp": lax.rem(m + k, count), "pipe": 1 - p},
            device_id_type=MESH,
        )
    pl.semaphore_wait(barrier, n - 1 + count - 1 + count)


def relay_kernel(
    x_hbm, up_hbm, down_hbm, head_hbm, layer_gain, final_gain, ids_ref, mask_ref, anchor_ref,
    pairs_ref, token_ref, policy_ref, loss_ref, full_ref, head, stats, tallies, up, down, xs, normed, xin, hid, act, ext, outs, rs, resid, nxt, slots, fin,
    load, go, ns, nr, xs_s, xs_r, gs, gr, ins, inr, exr, bs, br, rss, rsr, ds, dr, qs, qr,
    hs, hr, fs, fr, es, er, load_head, ts, tr, vs, vr,
):
    n, count = lax.axis_size("dp"), lax.axis_size("mp")
    d, m, p = lax.axis_index("dp"), lax.axis_index("mp"), lax.axis_index("pipe")
    length, width = x_hbm.shape
    block, ff = up.shape
    part = length // count
    sub = part // BATCHES
    own_rows = sub * n
    batch = own_rows * count
    half = batch // 2
    piece = half // PIECES
    total = BATCHES * PIECES
    f32 = jnp.float32

    def rows(start, size):
        return pl.ds(pl.multiple_of(start, 16), size)

    def columns(owner):
        return pl.ds(pl.multiple_of(owner * block, 128), block)

    loads = [
        pltpu.make_async_copy(x_hbm.at[rows(m * part, part)], xs, load.at[0]),
        pltpu.make_async_copy(up_hbm, up, load.at[1]),
        pltpu.make_async_copy(down_hbm, down, load.at[2]),
    ]
    for copy in loads:
        copy.start()
    meet()
    seq_count, seq_len = mask_ref.shape

    def flat(ref):
        return jnp.concatenate([ref[s : s + 1, :] for s in range(seq_count)], axis=1)

    lanes = lax.broadcasted_iota(jnp.int32, (length, 128), 1)
    member = (lanes == lax.broadcasted_iota(jnp.int32, (length, 128), 0) // seq_len).astype(f32)

    def per_sequence(row):
        return lax.dot_general(
            jnp.broadcast_to(row, (8, length)),
            member,
            (((1,), (0,)), ((), ())),
            precision=lax.Precision.HIGHEST,
            preferred_element_type=f32,
        )

    mask = flat(mask_ref).astype(f32)
    tallies[0] = per_sequence(mask)

    def tally(k):
        return remote(
            tallies.at[0], tallies.at[k], ts.at[k], tr.at[k], {"dp": lax.rem(d + k, n)}
        )

    loads[0].wait()

    def first_hop(b, k, owner):
        to = lax.rem(d + k, n)
        return remote(
            normed.at[rows(b * sub, sub), columns(to)],
            xin.at[rows(b * batch + (m * n + owner) * sub, sub)],
            ns.at[b, k],
            nr.at[b, k],
            {"dp": to},
        )

    def plain_hop(b, k, owner):
        to = lax.rem(d + k, n)
        return remote(
            xs.at[rows(b * sub, sub), columns(to)],
            resid.at[rows(b * own_rows + owner * sub, sub)],
            xs_s.at[b, k],
            xs_r.at[b, k],
            {"dp": to},
        )

    def share(b, k, owner):
        slab = xin.at[rows(b * batch + owner * own_rows, own_rows)]
        return remote(slab, slab, gs.at[b, k], gr.at[b, k], {"mp": lax.rem(m + k, count)})

    def scatter(b, k):
        to = lax.rem(m + k, count)
        return remote(
            outs.at[rows(b * batch + to * own_rows, own_rows)],
            rs.at[rows((b * count + k) * own_rows, own_rows)],
            rss.at[b, k],
            rsr.at[b, k],
            {"mp": to, "pipe": 1 - p},
        )

    def hand_over(b):
        slab = rows(b * own_rows, own_rows)
        return remote(nxt.at[slab], resid.at[slab], ds.at[b], dr.at[b], {"pipe": 1 - p})

    def square(b, k):
        return remote(
            slots.at[b, 0], slots.at[b, k], qs.at[b, k], qr.at[b, k], {"dp": lax.rem(d + k, n)}
        )

    def last_hop(b, k, owner):
        to = lax.rem(d + k, n)
        return remote(
            nxt.at[rows(b * own_rows + to * sub, sub)],
            fin.at[b, owner],
            hs.at[b, k],
            hr.at[b, k],
            {"dp": to},
        )

    def spot(b, owner):
        return full_ref.at[rows(owner * part + b * sub, sub)]

    def full_share(b, k, owner):
        return remote(
            spot(b, owner), spot(b, owner), fs.at[b, k], fr.at[b, k], {"mp": lax.rem(m + k, count)}
        )

    def full_pass(b, k):
        owner = lax.rem(m - k + count, count)
        return remote(
            spot(b, owner), spot(b, owner), es.at[b, k], er.at[b, k], {"pipe": 1 - p}
        )

    def before(k):
        return lax.rem(d - k + n, n)

    def beside(k):
        return lax.rem(m - k + count, count)

    @pl.when(p == 0)
    def _():
        wide = xs[...].astype(f32)
        scale = lax.rsqrt(jnp.mean(wide * wide, axis=-1, keepdims=True) + epsilon)
        normed[...] = (wide * scale * layer_gain[...]).astype(normed.dtype)
        for b in range(BATCHES):
            for k in range(1, n):
                first_hop(b, k, d).start()
        for b in range(BATCHES):
            xin[rows(b * batch + (m * n + d) * sub, sub), :] = normed[
                b * sub : (b + 1) * sub, columns(d)
            ]
        for b in range(BATCHES):
            for k in range(1, n):
                first_hop(b, k, before(k)).wait_recv()
            for k in range(1, count):
                share(b, k, m).start()
        pl.semaphore_signal(go, inc=1, device_id={"pipe": 1 - p}, device_id_type=MESH)

    @pl.when(p == 1)
    def _():
        pl.semaphore_wait(go, 1)
        for b in range(BATCHES):
            for k in range(1, n):
                plain_hop(b, k, d).start()
            resid[rows(b * own_rows + d * sub, sub), :] = xs[b * sub : (b + 1) * sub, columns(d)]

    for k in range(1, n):
        tally(k).start()
    loads[1].wait()
    loads[2].wait()
    slots_head, tall, _ = head.shape
    vocab = head_hbm.shape[0]

    def head_load(j):
        return pltpu.make_async_copy(
            head_hbm.at[pl.ds(j * tall, tall)],
            head.at[j % slots_head],
            load_head.at[j % slots_head],
        )

    for j in range(slots_head):
        head_load(j).start()

    def enter(b):
        for k in range(1, count):
            share(b, k, beside(k)).wait_recv()
        where = rows(b * batch, batch)
        states = xin[where, :]
        step = 256
        for j in range(0, ff, step):
            hid[where, j : j + step] = jnp.dot(
                states, up[:, j : j + step], preferred_element_type=f32
            ).astype(hid.dtype)

    def leave(b):
        where = rows(b * batch, batch)
        states = act[where, :]
        step = min(block, 256)
        for j in range(0, block, step):
            outs[where, j : j + step] = jnp.dot(
                states, down[:, j : j + step], preferred_element_type=f32
            ).astype(outs.dtype)
        for k in (*range(1, count), 0):
            scatter(b, k).start()

    def add_up(b):
        for k in range(count):
            scatter(b, k).wait_recv()
        slab = rows(b * own_rows, own_rows)
        value = resid[slab, :].astype(f32)
        for k in range(count):
            value = value + rs[rows((b * count + k) * own_rows, own_rows), :].astype(f32)
        value = value.astype(nxt.dtype)
        nxt[slab, :] = value
        return value.astype(f32)

    def settle(b):
        for k in range(1, n):
            plain_hop(b, k, before(k)).wait_recv()
        wide = add_up(b)
        sums = jnp.sum(wide * wide, axis=1, keepdims=True)
        slots[b, 0] = jnp.broadcast_to(sums, (own_rows, 128))
        for k in range(1, n):
            square(b, k).start()
        hand_over(b).start()

    def renew(b):
        sums = slots[b, 0]
        for k in range(1, n):
            square(b, k).wait_recv()
            sums = sums + slots[b, k]
        scale = lax.rsqrt(sums[:, :1] / width + epsilon)
        wide = nxt[rows(b * own_rows, own_rows), :].astype(f32)
        gain = layer_gain[:, columns(d)]
        xin[rows(b * batch + m * own_rows, own_rows), :] = (wide * scale * gain).astype(xin.dtype)
        for k in range(1, count):
            share(b, k, m).start()

    def span(way, c):
        b, k = lax.div(c, PIECES), lax.rem(c, PIECES)
        return rows(b * batch + way * half + k * piece, piece)

    def inner(way, c, to, into, sem):
        return remote(hid.at[span(way, c)], into, ins.at[way, c], sem.at[way, c], {"dp": to})

    def to_act(way, c, to):
        return inner(way, c, to, act.at[span(way, c)], inr)

    def to_ext(way, c, to):
        return inner(way, c, to, ext.at[rows(c * piece, piece)], exr)

    def outer(way, c, side):
        where = act.at[span(way, c)]
        to = d - 1 if side == 0 else d + 1
        return remote(where, where, bs.at[way, c, side], br.at[way, c], {"dp": to})

    offset = 2 * STEP + 1
    deep = HOP * (n // 2)
    ticks = offset + total + 2 * deep

    def tick(t, carry):
        now = t - offset
        for way in range(2):
            owner = n // 2 - way
            left, right = d < owner, d > owner
            hops = jnp.where(left, d, n - 1 - d)
            c = now - HOP * hops

            @pl.when((d != owner) & (c >= 0) & (c < total))
            def _():
                here = span(way, c)

                @pl.when(hops > 0)
                def _():
                    to_act(way, c, d).wait_recv()
                    for j in range(0, ff, 256):
                        cut = slice(j, j + 256)
                        hid[here, cut] = (
                            hid[here, cut].astype(f32) + act[here, cut].astype(f32)
                        ).astype(hid.dtype)

                @pl.when(left)
                def _():
                    to_act(way, c, d + 1).start()

                @pl.when(right & (d - 1 > owner))
                def _():
                    to_act(way, c, d - 1).start()

                @pl.when(right & (d - 1 == owner))
                def _():
                    to_ext(way, c, d - 1).start()

        for way in range(2):
            owner = n // 2 - way
            c = now - deep

            @pl.when((d == owner) & (c >= 0) & (c < total))
            def _():
                here = span(way, c)
                there = rows(c * piece, piece)
                if owner > 0:
                    to_act(way, c, d).wait_recv()
                if owner < n - 1:
                    to_ext(way, c, d).wait_recv()
                for j in range(0, ff, 256):
                    cut = slice(j, j + 256)
                    value = hid[here, cut].astype(f32)
                    if owner > 0:
                        value = value + act[here, cut].astype(f32)
                    if owner < n - 1:
                        value = value + ext[there, cut].astype(f32)
                    act[here, cut] = (value / (1.0 + jnp.exp(-value))).astype(act.dtype)
                if owner > 0:
                    outer(way, c, 0).start()
                if owner < n - 1:
                    outer(way, c, 1).start()

        for way in range(2):
            owner = n // 2 - way
            left, right = d < owner, d > owner
            away = jnp.where(left, owner - d, d - owner)
            c = now - deep - HOP * away

            @pl.when((d != owner) & (c >= 0) & (c < total))
            def _():
                outer(way, c, 0).wait_recv()

                @pl.when(left & (d > 0))
                def _():
                    outer(way, c, 0).start()

                @pl.when(right & (d < n - 1))
                def _():
                    outer(way, c, 1).start()

        b = lax.div(now + 1, PIECES)

        @pl.when((now + 1 >= 0) & (lax.rem(now + 1, PIECES) == 0) & (b < BATCHES))
        def _():
            enter(b)

        done = now - (PIECES - 1) - 2 * deep
        q = lax.div(done, PIECES)

        @pl.when((done >= 0) & (lax.rem(done, PIECES) == 0) & (q < BATCHES))
        def _():
            leave(q)

        late = now + 1 + STEP
        e = lax.div(late, PIECES)

        @pl.when((p == 1) & (late >= 0) & (lax.rem(late, PIECES) == 0) & (e < BATCHES))
        def _():
            renew(e)

        early = now + 1 + 2 * STEP
        a = lax.div(early, PIECES)

        @pl.when((p == 1) & (lax.rem(early, PIECES) == 0) & (a < BATCHES))
        def _():
            settle(a)

        return carry

    lax.fori_loop(0, ticks, tick, 0)

    @pl.when(p == 0)
    def _():
        def finish(b, carry):
            hand_over(b).wait_recv()
            add_up(b)
            for k in range(1, n):
                last_hop(b, k, d).start()
            fin[b, d] = nxt[rows(b * own_rows + d * sub, sub), :]
            for k in range(1, n):
                last_hop(b, k, before(k)).wait_recv()
            sums = 0.0
            for g in range(n):
                wide = fin[b, g].astype(f32)
                sums = sums + jnp.sum(wide * wide, axis=1, keepdims=True)
            scale = lax.rsqrt(sums / width + epsilon)
            for g in range(n):
                cut = slice(g * block, (g + 1) * block)
                full_ref[rows(m * part + b * sub, sub), cut] = (
                    fin[b, g].astype(f32) * scale * final_gain[:, cut]
                ).astype(full_ref.dtype)
            for k in range(1, count):
                full_share(b, k, m).start()
            full_pass(b, 0).start()
            for k in range(1, count):
                full_share(b, k, beside(k)).wait_recv()
                full_pass(b, k).start()
            return carry

        lax.fori_loop(0, BATCHES, finish, 0)

    @pl.when(p == 1)
    def _():
        def finish(b, carry):
            for k in range(count):
                full_pass(b, k).wait_recv()
            return carry

        lax.fori_loop(0, BATCHES, finish, 0)

    states = full_ref[...]
    ids = flat(ids_ref) - (p * count + m) * vocab
    spots = lax.broadcasted_iota(jnp.int32, (tall, length), 0)
    top = jnp.full((1, length), -jnp.inf, f32)
    mass = jnp.zeros((1, length), f32)
    picked = jnp.zeros((1, length), f32)

    def gauge(j, logits, carry):
        top, mass, picked = carry
        peak = jnp.maximum(top, jnp.max(logits, axis=0, keepdims=True))
        mass = mass * jnp.exp(top - peak) + jnp.sum(jnp.exp(logits - peak), axis=0, keepdims=True)
        hit = jnp.where(spots == ids - j * tall, logits, 0.0)
        return peak, mass, picked + jnp.sum(hit, axis=0, keepdims=True)

    carry = top, mass, picked
    last = None
    for j in range(vocab // tall):
        head_load(j).wait()
        logits = lax.dot_general(
            head[j % slots_head],
            states,
            (((1,), (1,)), ((), ())),
            preferred_element_type=f32,
        )
        if j + slots_head < vocab // tall:
            head_load(j + slots_head).start()
        if last is not None:
            carry = gauge(j - 1, last, carry)
        last = logits
    top, mass, picked = gauge(vocab // tall - 1, last, carry)

    def report(q, k):
        to = {"mp": lax.rem(m + k, count), "pipe": (p if q == 0 else 1 - p)}
        slot = q * count + k
        return remote(stats.at[0], stats.at[slot], vs.at[slot], vr.at[slot], to)

    others = [(q, k) for k in range(1, count) for q in range(2)] + [(1, 0)]
    stats[0] = jnp.concatenate([top, mass, picked, jnp.zeros((5, length), f32)], axis=0)
    for q, k in others:
        report(q, k).start()
    tallied = tallies[0]
    for k in range(1, n):
        tally(k).wait_recv()
        tallied = tallied + tallies[k]
    for q, k in others:
        report(q, k).wait_recv()
    peak = jnp.max(stats[:, 0, :], axis=0, keepdims=True)
    mass = jnp.sum(stats[:, 1, :] * jnp.exp(stats[:, 0, :] - peak), axis=0, keepdims=True)
    picked = jnp.sum(stats[:, 2, :], axis=0, keepdims=True)
    token = picked - peak - jnp.log(mass)
    for s in range(seq_count):
        token_ref[s : s + 1, :] = token[:, s * seq_len : (s + 1) * seq_len]
    lane = lax.broadcasted_iota(jnp.int32, (8, 128), 1)
    divisor = jnp.where(lane < seq_count, tallied / (n * SEQ_MB), 1.0)
    policy = per_sequence(mask * token) / divisor
    anchor = per_sequence(mask * flat(anchor_ref)) / divisor
    gaps = policy - anchor
    policy_ref[...] = policy[:1, :seq_count]
    losses = jnp.zeros((8, 128), f32)
    for i in range(seq_count // 2):
        chosen = jnp.sum(
            jnp.where(lane == pairs_ref[0, 2 * i], gaps, 0.0), axis=1, keepdims=True
        )
        rejected = jnp.sum(
            jnp.where(lane == pairs_ref[0, 2 * i + 1], gaps, 0.0), axis=1, keepdims=True
        )
        losses = jnp.where(lane == i, (chosen - rejected - 0.5 / ipo_tau) ** 2, losses)
    loss_ref[...] = losses[:1, : seq_count // 2]
    for k in range(1, n):
        tally(k).wait_send()
    for q, k in others:
        report(q, k).wait_send()

    def drain(b, carry):
        for k in range(1, count):
            share(b, k, m).wait_send()
        for k in range(count):
            scatter(b, k).wait_send()

        @pl.when(p == 0)
        def _():
            for k in range(1, n):
                first_hop(b, k, d).wait_send()
                last_hop(b, k, d).wait_send()
            for k in range(1, count):
                full_share(b, k, m).wait_send()
            for k in range(count):
                full_pass(b, k).wait_send()

        @pl.when(p == 1)
        def _():
            for k in range(1, n):
                plain_hop(b, k, d).wait_send()
                square(b, k).wait_send()
            hand_over(b).wait_send()

        return carry

    lax.fori_loop(0, BATCHES, drain, 0)

    def drain_pieces(c, carry):
        for way in range(2):
            owner = n // 2 - way

            @pl.when(d != owner)
            def _():
                to_act(way, c, d).wait_send()

            @pl.when((d <= owner) & (d > 0))
            def _():
                outer(way, c, 0).wait_send()

            @pl.when((d >= owner) & (d < n - 1))
            def _():
                outer(way, c, 1).wait_send()

        return carry

    lax.fori_loop(0, total, drain_pieces, 0)


def sems(*shape):
    return [pltpu.SemaphoreType.DMA(shape)] * 2


def shards(
    hidden_states,
    up_weight,
    down_weight,
    layer_gain,
    final_gain,
    unembedding,
    target_ids,
    response_masks,
    anchor_logps,
    pairing,
):
    seq_count, length, model_width = hidden_states.shape
    groups = lax.axis_size("dp")
    vp_size = lax.axis_size("pipe") * lax.axis_size("mp")
    rows = seq_count * length
    block = model_width // groups
    ff = up_weight.shape[2]
    count = lax.axis_size("mp")
    bf16 = jnp.bfloat16
    part = rows // count
    own_rows = part * groups
    all_rows = rows * groups
    steps = BATCHES * PIECES
    vocab = unembedding.shape[0]
    anyspec = pl.BlockSpec(memory_space=pl.ANY)
    spec = pl.BlockSpec(memory_space=pltpu.VMEM)
    smem = pl.BlockSpec(memory_space=pltpu.SMEM)
    dma = pltpu.SemaphoreType.DMA
    buffers = [
        ((rows, model_width), bf16),
        None,
        ((vp_size, 8, rows), jnp.float32),
        ((groups, 8, 128), jnp.float32),
        ((block, ff), bf16),
        ((ff, block), bf16),
        ((part, model_width), bf16),
        ((part, model_width), bf16),
        ((all_rows, block), bf16),
        ((all_rows, ff), bf16),
        ((all_rows, ff), bf16),
        ((all_rows // 2, ff), bf16),
        ((all_rows, block), bf16),
        ((all_rows, block), bf16),
        ((own_rows, block), bf16),
        ((own_rows, block), bf16),
        ((BATCHES, groups, own_rows // BATCHES, 128), jnp.float32),
        ((BATCHES, groups, part // BATCHES, block), bf16),
    ]
    used = sum(math.prod(b[0]) * jnp.dtype(b[1]).itemsize for b in buffers if b)
    tall = vocab // 8
    kept = min(8, (ROOM - used) // (tall * model_width * 2))
    buffers[1] = ((kept, tall, model_width), bf16)
    token_logps, policy, losses = pl.pallas_call(
        relay_kernel,
        name="relay",
        out_shape=[
            jax.ShapeDtypeStruct(target_ids.shape, jnp.float32),
            jax.ShapeDtypeStruct((1, seq_count), jnp.float32),
            jax.ShapeDtypeStruct((1, seq_count // 2), jnp.float32),
        ],
        in_specs=[anyspec] * 4 + [spec] * 5 + [smem],
        out_specs=[spec] * 3,
        scratch_shapes=[pltpu.VMEM(*b) for b in buffers]
        + [dma((3,)), pltpu.SemaphoreType.REGULAR]
        + sems(BATCHES, groups)
        + sems(BATCHES, groups)
        + sems(BATCHES, count)
        + [dma((2, steps))] * 3
        + [dma((2, steps, 2)), dma((2, steps))]
        + sems(BATCHES, count)
        + sems(BATCHES)
        + sems(BATCHES, groups)
        + sems(BATCHES, groups)
        + sems(BATCHES, count)
        + sems(BATCHES, count)
        + [dma((kept,))]
        + sems(groups)
        + sems(vp_size),
        compiler_params=pltpu.CompilerParams(
            collective_id=0, has_side_effects=True, vmem_limit_bytes=67043328
        ),
    )(
        hidden_states.reshape(rows, model_width),
        up_weight[0],
        down_weight[0],
        unembedding,
        layer_gain,
        final_gain[None],
        target_ids,
        response_masks,
        anchor_logps,
        pairing,
    )
    return token_logps, policy[0], losses[0]


def solution(mesh):
    return jax.shard_map(
        shards,
        mesh=mesh,
        in_specs=(
            P("dp", None, None),
            P("pipe", "dp", "mp"),
            P("pipe", "mp", "dp"),
            P("pipe", None),
            P(),
            P(("pipe", "mp"), None),
            P("dp", None),
            P("dp", None),
            P("dp", None),
            P("dp", None),
        ),
        out_specs=(P("dp", None), P("dp"), P("dp")),
        check_vma=False,
    )
```

```python
import math
import jax
import jax.numpy as jnp
from jax import lax
from jax.experimental import pallas as pl
from jax.experimental.pallas import tpu as pltpu
from jax.sharding import PartitionSpec as P

SEQ_MB = 1

epsilon = 1e-05
ipo_tau = 0.5
MESH = pl.DeviceIdType.MESH
BATCHES = 4
PIECES = 4
ROUND = 2 * PIECES
HOP = 3
STEP = 4
ROOM = 62 * 1024 * 1024


def remote(src, dst, send_sem, recv_sem, target):
    return pltpu.make_async_remote_copy(
        src_ref=src,
        dst_ref=dst,
        send_sem=send_sem,
        recv_sem=recv_sem,
        device_id=target,
        device_id_type=MESH,
    )


def meet():
    barrier = pltpu.get_barrier_semaphore()
    n, count = lax.axis_size("dp"), lax.axis_size("mp")
    d, m, p = lax.axis_index("dp"), lax.axis_index("mp"), lax.axis_index("pipe")
    for k in range(1, n):
        pl.semaphore_signal(
            barrier, inc=1, device_id={"dp": lax.rem(d + k, n)}, device_id_type=MESH
        )
    for k in range(1, count):
        pl.semaphore_signal(
            barrier, inc=1, device_id={"mp": lax.rem(m + k, count)}, device_id_type=MESH
        )
    for k in range(count):
        pl.semaphore_signal(
            barrier,
            inc=1,
            device_id={"mp": lax.rem(m + k, count), "pipe": 1 - p},
            device_id_type=MESH,
        )
    pl.semaphore_wait(barrier, n - 1 + count - 1 + count)


def relay_kernel(
    x_hbm, up_hbm, down_hbm, head_hbm, layer_gain, final_gain, ids_ref, mask_ref, anchor_ref,
    pairs_ref, token_ref, policy_ref, loss_ref, full_ref, head, stats, tallies, up, down, xs, normed, xin, hid, act, ext, outs, rs, resid, nxt, slots, fin,
    load, go, ns, nr, xs_s, xs_r, gs, gr, ins, inr, exr, bs, br, rss, rsr, ds, dr, qs, qr,
    hs, hr, fs, fr, es, er, load_head, ts, tr, vs, vr,
):
    n, count = lax.axis_size("dp"), lax.axis_size("mp")
    d, m, p = lax.axis_index("dp"), lax.axis_index("mp"), lax.axis_index("pipe")
    length, width = x_hbm.shape
    block, ff = up.shape
    part = length // count
    sub = part // BATCHES
    own_rows = sub * n
    batch = own_rows * count
    half = batch // 2
    piece = half // PIECES
    total = BATCHES * PIECES
    f32 = jnp.float32

    def rows(start, size):
        return pl.ds(pl.multiple_of(start, 16), size)

    def columns(owner):
        return pl.ds(pl.multiple_of(owner * block, 128), block)

    loads = [
        pltpu.make_async_copy(x_hbm.at[rows(m * part, part)], xs, load.at[0]),
        pltpu.make_async_copy(up_hbm, up, load.at[1]),
        pltpu.make_async_copy(down_hbm, down, load.at[2]),
    ]
    for copy in loads:
        copy.start()
    meet()
    seq_count, seq_len = mask_ref.shape

    def flat(ref):
        return jnp.concatenate([ref[s : s + 1, :] for s in range(seq_count)], axis=1)

    lanes = lax.broadcasted_iota(jnp.int32, (length, 128), 1)
    member = (lanes == lax.broadcasted_iota(jnp.int32, (length, 128), 0) // seq_len).astype(f32)

    def per_sequence(row):
        return lax.dot_general(
            jnp.broadcast_to(row, (8, length)),
            member,
            (((1,), (0,)), ((), ())),
            precision=lax.Precision.HIGHEST,
            preferred_element_type=f32,
        )

    mask = flat(mask_ref).astype(f32)
    tallies[0] = per_sequence(mask)

    def tally(k):
        return remote(
            tallies.at[0], tallies.at[k], ts.at[k], tr.at[k], {"dp": lax.rem(d + k, n)}
        )

    loads[0].wait()

    def first_hop(b, k, owner):
        to = lax.rem(d + k, n)
        return remote(
            normed.at[rows(b * sub, sub), columns(to)],
            xin.at[rows(b * batch + (m * n + owner) * sub, sub)],
            ns.at[b, k],
            nr.at[b, k],
            {"dp": to},
        )

    def plain_hop(b, k, owner):
        to = lax.rem(d + k, n)
        return remote(
            xs.at[rows(b * sub, sub), columns(to)],
            resid.at[rows(b * own_rows + owner * sub, sub)],
            xs_s.at[b, k],
            xs_r.at[b, k],
            {"dp": to},
        )

    def share(b, k, owner):
        slab = xin.at[rows(b * batch + owner * own_rows, own_rows)]
        return remote(slab, slab, gs.at[b, k], gr.at[b, k], {"mp": lax.rem(m + k, count)})

    def scatter(b, k):
        to = lax.rem(m + k, count)
        return remote(
            outs.at[rows(b * batch + to * own_rows, own_rows)],
            rs.at[rows((b * count + k) * own_rows, own_rows)],
            rss.at[b, k],
            rsr.at[b, k],
            {"mp": to, "pipe": 1 - p},
        )

    def hand_over(b):
        slab = rows(b * own_rows, own_rows)
        return remote(nxt.at[slab], resid.at[slab], ds.at[b], dr.at[b], {"pipe": 1 - p})

    def square(b, k):
        return remote(
            slots.at[b, 0], slots.at[b, k], qs.at[b, k], qr.at[b, k], {"dp": lax.rem(d + k, n)}
        )

    def last_hop(b, k, owner):
        to = lax.rem(d + k, n)
        return remote(
            nxt.at[rows(b * own_rows + to * sub, sub)],
            fin.at[b, owner],
            hs.at[b, k],
            hr.at[b, k],
            {"dp": to},
        )

    def spot(b, owner):
        return full_ref.at[rows(owner * part + b * sub, sub)]

    def full_share(b, k, owner):
        return remote(
            spot(b, owner), spot(b, owner), fs.at[b, k], fr.at[b, k], {"mp": lax.rem(m + k, count)}
        )

    def full_pass(b, k):
        owner = lax.rem(m - k + count, count)
        return remote(
            spot(b, owner), spot(b, owner), es.at[b, k], er.at[b, k], {"pipe": 1 - p}
        )

    def before(k):
        return lax.rem(d - k + n, n)

    def beside(k):
        return lax.rem(m - k + count, count)

    @pl.when(p == 0)
    def _():
        wide = xs[...].astype(f32)
        scale = lax.rsqrt(jnp.mean(wide * wide, axis=-1, keepdims=True) + epsilon)
        normed[...] = (wide * scale * layer_gain[...]).astype(normed.dtype)
        for b in range(BATCHES):
            for k in range(1, n):
                first_hop(b, k, d).start()
        for b in range(BATCHES):
            xin[rows(b * batch + (m * n + d) * sub, sub), :] = normed[
                b * sub : (b + 1) * sub, columns(d)
            ]
        for b in range(BATCHES):
            for k in range(1, n):
                first_hop(b, k, before(k)).wait_recv()
            for k in range(1, count):
                share(b, k, m).start()
        pl.semaphore_signal(go, inc=1, device_id={"pipe": 1 - p}, device_id_type=MESH)

    @pl.when(p == 1)
    def _():
        pl.semaphore_wait(go, 1)
        for b in range(BATCHES):
            for k in range(1, n):
                plain_hop(b, k, d).start()
            resid[rows(b * own_rows + d * sub, sub), :] = xs[b * sub : (b + 1) * sub, columns(d)]

    for k in range(1, n):
        tally(k).start()
    loads[1].wait()
    loads[2].wait()
    slots_head, tall, _ = head.shape
    vocab = head_hbm.shape[0]

    def head_load(j):
        return pltpu.make_async_copy(
            head_hbm.at[pl.ds(j * tall, tall)],
            head.at[j % slots_head],
            load_head.at[j % slots_head],
        )

    for j in range(slots_head):
        head_load(j).start()

    def enter(b):
        for k in range(1, count):
            share(b, k, beside(k)).wait_recv()
        where = rows(b * batch, batch)
        states = xin[where, :]
        hid[where, :] = jnp.dot(states, up[...], preferred_element_type=f32).astype(hid.dtype)

    def leave(b):
        where = rows(b * batch, batch)
        states = act[where, :]
        outs[where, :] = jnp.dot(states, down[...], preferred_element_type=f32).astype(outs.dtype)
        for k in (*range(1, count), 0):
            scatter(b, k).start()

    def add_up(b):
        for k in range(count):
            scatter(b, k).wait_recv()
        slab = rows(b * own_rows, own_rows)
        value = resid[slab, :].astype(f32)
        for k in range(count):
            value = value + rs[rows((b * count + k) * own_rows, own_rows), :].astype(f32)
        value = value.astype(nxt.dtype)
        nxt[slab, :] = value
        return value.astype(f32)

    def settle(b):
        for k in range(1, n):
            plain_hop(b, k, before(k)).wait_recv()
        wide = add_up(b)
        sums = jnp.sum(wide * wide, axis=1, keepdims=True)
        slots[b, 0] = jnp.broadcast_to(sums, (own_rows, 128))
        for k in range(1, n):
            square(b, k).start()
        hand_over(b).start()

    def renew(b):
        sums = slots[b, 0]
        for k in range(1, n):
            square(b, k).wait_recv()
            sums = sums + slots[b, k]
        scale = lax.rsqrt(sums[:, :1] / width + epsilon)
        wide = nxt[rows(b * own_rows, own_rows), :].astype(f32)
        gain = layer_gain[:, columns(d)]
        xin[rows(b * batch + m * own_rows, own_rows), :] = (wide * scale * gain).astype(xin.dtype)
        for k in range(1, count):
            share(b, k, m).start()

    def span(way, c):
        b, k = lax.div(c, PIECES), lax.rem(c, PIECES)
        return rows(b * batch + way * half + k * piece, piece)

    def inner(way, c, to, into, sem):
        return remote(hid.at[span(way, c)], into, ins.at[way, c], sem.at[way, c], {"dp": to})

    def to_act(way, c, to):
        return inner(way, c, to, act.at[span(way, c)], inr)

    def to_ext(way, c, to):
        return inner(way, c, to, ext.at[rows(c * piece, piece)], exr)

    def outer(way, c, side):
        where = act.at[span(way, c)]
        to = d - 1 if side == 0 else d + 1
        return remote(where, where, bs.at[way, c, side], br.at[way, c], {"dp": to})

    offset = 2 * STEP + 1
    deep = HOP * (n // 2)
    ticks = offset + 2 * total + 2 * deep

    def tick(t, carry):
        now = t - offset
        for way in range(2):
            owner = n // 2 - way
            left, right = d < owner, d > owner
            hops = jnp.where(left, d, n - 1 - d)
            late = now - way - HOP * hops
            c = lax.div(late, 2)

            @pl.when((d != owner) & (late >= 0) & (lax.rem(late, 2) == 0) & (c < total))
            def _():
                here = span(way, c)

                @pl.when(hops > 0)
                def _():
                    to_act(way, c, d).wait_recv()
                    for j in range(0, ff, 256):
                        cut = slice(j, j + 256)
                        hid[here, cut] = (
                            hid[here, cut].astype(f32) + act[here, cut].astype(f32)
                        ).astype(hid.dtype)

                @pl.when(left)
                def _():
                    to_act(way, c, d + 1).start()

                @pl.when(right & (d - 1 > owner))
                def _():
                    to_act(way, c, d - 1).start()

                @pl.when(right & (d - 1 == owner))
                def _():
                    to_ext(way, c, d - 1).start()

        for way in range(2):
            owner = n // 2 - way
            late = now - way - deep
            c = lax.div(late, 2)

            @pl.when((d == owner) & (late >= 0) & (lax.rem(late, 2) == 0) & (c < total))
            def _():
                here = span(way, c)
                there = rows(c * piece, piece)
                if owner > 0:
                    to_act(way, c, d).wait_recv()
                if owner < n - 1:
                    to_ext(way, c, d).wait_recv()
                for j in range(0, ff, 256):
                    cut = slice(j, j + 256)
                    value = hid[here, cut].astype(f32)
                    if owner > 0:
                        value = value + act[here, cut].astype(f32)
                    if owner < n - 1:
                        value = value + ext[there, cut].astype(f32)
                    act[here, cut] = (value / (1.0 + jnp.exp(-value))).astype(act.dtype)
                if owner > 0:
                    outer(way, c, 0).start()
                if owner < n - 1:
                    outer(way, c, 1).start()

        for way in range(2):
            owner = n // 2 - way
            left, right = d < owner, d > owner
            away = jnp.where(left, owner - d, d - owner)
            late = now - way - deep - HOP * away
            c = lax.div(late, 2)

            @pl.when((d != owner) & (late >= 0) & (lax.rem(late, 2) == 0) & (c < total))
            def _():
                outer(way, c, 0).wait_recv()

                @pl.when(left & (d > 0))
                def _():
                    outer(way, c, 0).start()

                @pl.when(right & (d < n - 1))
                def _():
                    outer(way, c, 1).start()

        b = lax.div(now + 1, ROUND)

        @pl.when((now + 1 >= 0) & (lax.rem(now + 1, ROUND) == 0) & (b < BATCHES))
        def _():
            enter(b)

        done = now - (ROUND - 1) - 2 * deep
        q = lax.div(done, ROUND)

        @pl.when((done >= 0) & (lax.rem(done, ROUND) == 0) & (q < BATCHES))
        def _():
            leave(q)

        late = now + 1 + STEP
        e = lax.div(late, ROUND)

        @pl.when((p == 1) & (late >= 0) & (lax.rem(late, ROUND) == 0) & (e < BATCHES))
        def _():
            renew(e)

        early = now + 1 + 2 * STEP
        a = lax.div(early, ROUND)

        @pl.when((p == 1) & (lax.rem(early, ROUND) == 0) & (a < BATCHES))
        def _():
            settle(a)

        return carry

    lax.fori_loop(0, ticks, tick, 0)

    @pl.when(p == 0)
    def _():
        def finish(b, carry):
            hand_over(b).wait_recv()
            add_up(b)
            for k in range(1, n):
                last_hop(b, k, d).start()
            fin[b, d] = nxt[rows(b * own_rows + d * sub, sub), :]
            for k in range(1, n):
                last_hop(b, k, before(k)).wait_recv()
            sums = 0.0
            for g in range(n):
                wide = fin[b, g].astype(f32)
                sums = sums + jnp.sum(wide * wide, axis=1, keepdims=True)
            scale = lax.rsqrt(sums / width + epsilon)
            for g in range(n):
                cut = slice(g * block, (g + 1) * block)
                full_ref[rows(m * part + b * sub, sub), cut] = (
                    fin[b, g].astype(f32) * scale * final_gain[:, cut]
                ).astype(full_ref.dtype)
            for k in range(1, count):
                full_share(b, k, m).start()
            full_pass(b, 0).start()
            for k in range(1, count):
                full_share(b, k, beside(k)).wait_recv()
                full_pass(b, k).start()
            return carry

        lax.fori_loop(0, BATCHES, finish, 0)

    @pl.when(p == 1)
    def _():
        def finish(b, carry):
            for k in range(count):
                full_pass(b, k).wait_recv()
            return carry

        lax.fori_loop(0, BATCHES, finish, 0)

    states = full_ref[...]
    ids = flat(ids_ref) - (p * count + m) * vocab
    spots = lax.broadcasted_iota(jnp.int32, (tall, length), 0)
    top = jnp.full((1, length), -jnp.inf, f32)
    mass = jnp.zeros((1, length), f32)
    picked = jnp.zeros((1, length), f32)

    def gauge(j, logits, carry):
        top, mass, picked = carry
        peak = jnp.maximum(top, jnp.max(logits, axis=0, keepdims=True))
        mass = mass * jnp.exp(top - peak) + jnp.sum(jnp.exp(logits - peak), axis=0, keepdims=True)
        hit = jnp.where(spots == ids - j * tall, logits, 0.0)
        return peak, mass, picked + jnp.sum(hit, axis=0, keepdims=True)

    carry = top, mass, picked
    last = None
    for j in range(vocab // tall):
        head_load(j).wait()
        logits = jnp.concatenate(
            [
                lax.dot_general(
                    head[j % slots_head, cut : cut + tall // 2],
                    states,
                    (((1,), (1,)), ((), ())),
                    preferred_element_type=f32,
                )
                for cut in (0, tall // 2)
            ],
            axis=0,
        )
        if j + slots_head < vocab // tall:
            head_load(j + slots_head).start()
        if last is not None:
            carry = gauge(j - 1, last, carry)
        last = logits
    top, mass, picked = gauge(vocab // tall - 1, last, carry)

    def report(q, k):
        to = {"mp": lax.rem(m + k, count), "pipe": (p if q == 0 else 1 - p)}
        slot = q * count + k
        return remote(stats.at[0], stats.at[slot], vs.at[slot], vr.at[slot], to)

    others = [(q, k) for k in range(1, count) for q in range(2)] + [(1, 0)]
    stats[0] = jnp.concatenate([top, mass, picked, jnp.zeros((5, length), f32)], axis=0)
    for q, k in others:
        report(q, k).start()
    tallied = tallies[0]
    for k in range(1, n):
        tally(k).wait_recv()
        tallied = tallied + tallies[k]
    for q, k in others:
        report(q, k).wait_recv()
    peak = jnp.max(stats[:, 0, :], axis=0, keepdims=True)
    mass = jnp.sum(stats[:, 1, :] * jnp.exp(stats[:, 0, :] - peak), axis=0, keepdims=True)
    picked = jnp.sum(stats[:, 2, :], axis=0, keepdims=True)
    token = picked - peak - jnp.log(mass)
    for s in range(seq_count):
        token_ref[s : s + 1, :] = token[:, s * seq_len : (s + 1) * seq_len]
    lane = lax.broadcasted_iota(jnp.int32, (8, 128), 1)
    divisor = jnp.where(lane < seq_count, tallied / (n * SEQ_MB), 1.0)
    policy = per_sequence(mask * token) / divisor
    anchor = per_sequence(mask * flat(anchor_ref)) / divisor
    gaps = policy - anchor
    policy_ref[...] = policy[:1, :seq_count]
    losses = jnp.zeros((8, 128), f32)
    for i in range(seq_count // 2):
        chosen = jnp.sum(
            jnp.where(lane == pairs_ref[0, 2 * i], gaps, 0.0), axis=1, keepdims=True
        )
        rejected = jnp.sum(
            jnp.where(lane == pairs_ref[0, 2 * i + 1], gaps, 0.0), axis=1, keepdims=True
        )
        losses = jnp.where(lane == i, (chosen - rejected - 0.5 / ipo_tau) ** 2, losses)
    loss_ref[...] = losses[:1, : seq_count // 2]
    for k in range(1, n):
        tally(k).wait_send()
    for q, k in others:
        report(q, k).wait_send()

    def drain(b, carry):
        for k in range(1, count):
            share(b, k, m).wait_send()
        for k in range(count):
            scatter(b, k).wait_send()

        @pl.when(p == 0)
        def _():
            for k in range(1, n):
                first_hop(b, k, d).wait_send()
                last_hop(b, k, d).wait_send()
            for k in range(1, count):
                full_share(b, k, m).wait_send()
            for k in range(count):
                full_pass(b, k).wait_send()

        @pl.when(p == 1)
        def _():
            for k in range(1, n):
                plain_hop(b, k, d).wait_send()
                square(b, k).wait_send()
            hand_over(b).wait_send()

        return carry

    lax.fori_loop(0, BATCHES, drain, 0)

    def drain_pieces(c, carry):
        for way in range(2):
            owner = n // 2 - way

            @pl.when(d != owner)
            def _():
                to_act(way, c, d).wait_send()

            @pl.when((d <= owner) & (d > 0))
            def _():
                outer(way, c, 0).wait_send()

            @pl.when((d >= owner) & (d < n - 1))
            def _():
                outer(way, c, 1).wait_send()

        return carry

    lax.fori_loop(0, total, drain_pieces, 0)


def sems(*shape):
    return [pltpu.SemaphoreType.DMA(shape)] * 2


def shards(
    hidden_states,
    up_weight,
    down_weight,
    layer_gain,
    final_gain,
    unembedding,
    target_ids,
    response_masks,
    anchor_logps,
    pairing,
):
    seq_count, length, model_width = hidden_states.shape
    groups = lax.axis_size("dp")
    vp_size = lax.axis_size("pipe") * lax.axis_size("mp")
    rows = seq_count * length
    block = model_width // groups
    ff = up_weight.shape[2]
    count = lax.axis_size("mp")
    bf16 = jnp.bfloat16
    part = rows // count
    own_rows = part * groups
    all_rows = rows * groups
    steps = BATCHES * PIECES
    vocab = unembedding.shape[0]
    anyspec = pl.BlockSpec(memory_space=pl.ANY)
    spec = pl.BlockSpec(memory_space=pltpu.VMEM)
    smem = pl.BlockSpec(memory_space=pltpu.SMEM)
    dma = pltpu.SemaphoreType.DMA
    buffers = [
        ((rows, model_width), bf16),
        None,
        ((vp_size, 8, rows), jnp.float32),
        ((groups, 8, 128), jnp.float32),
        ((block, ff), bf16),
        ((ff, block), bf16),
        ((part, model_width), bf16),
        ((part, model_width), bf16),
        ((all_rows, block), bf16),
        ((all_rows, ff), bf16),
        ((all_rows, ff), bf16),
        ((all_rows // 2, ff), bf16),
        ((all_rows, block), bf16),
        ((all_rows, block), bf16),
        ((own_rows, block), bf16),
        ((own_rows, block), bf16),
        ((BATCHES, groups, own_rows // BATCHES, 128), jnp.float32),
        ((BATCHES, groups, part // BATCHES, block), bf16),
    ]
    used = sum(math.prod(b[0]) * jnp.dtype(b[1]).itemsize for b in buffers if b)
    tall = vocab // 8
    kept = min(8, (ROOM - used) // (tall * model_width * 2))
    buffers[1] = ((kept, tall, model_width), bf16)
    token_logps, policy, losses = pl.pallas_call(
        relay_kernel,
        name="relay",
        out_shape=[
            jax.ShapeDtypeStruct(target_ids.shape, jnp.float32),
            jax.ShapeDtypeStruct((1, seq_count), jnp.float32),
            jax.ShapeDtypeStruct((1, seq_count // 2), jnp.float32),
        ],
        in_specs=[anyspec] * 4 + [spec] * 5 + [smem],
        out_specs=[spec] * 3,
        scratch_shapes=[pltpu.VMEM(*b) for b in buffers]
        + [dma((3,)), pltpu.SemaphoreType.REGULAR]
        + sems(BATCHES, groups)
        + sems(BATCHES, groups)
        + sems(BATCHES, count)
        + [dma((2, steps))] * 3
        + [dma((2, steps, 2)), dma((2, steps))]
        + sems(BATCHES, count)
        + sems(BATCHES)
        + sems(BATCHES, groups)
        + sems(BATCHES, groups)
        + sems(BATCHES, count)
        + sems(BATCHES, count)
        + [dma((kept,))]
        + sems(groups)
        + sems(vp_size),
        compiler_params=pltpu.CompilerParams(
            collective_id=0, has_side_effects=True, vmem_limit_bytes=67043328
        ),
    )(
        hidden_states.reshape(rows, model_width),
        up_weight[0],
        down_weight[0],
        unembedding,
        layer_gain,
        final_gain[None],
        target_ids,
        response_masks,
        anchor_logps,
        pairing,
    )
    return token_logps, policy[0], losses[0]


def solution(mesh):
    return jax.shard_map(
        shards,
        mesh=mesh,
        in_specs=(
            P("dp", None, None),
            P("pipe", "dp", "mp"),
            P("pipe", "mp", "dp"),
            P("pipe", None),
            P(),
            P(("pipe", "mp"), None),
            P("dp", None),
            P("dp", None),
            P("dp", None),
            P("dp", None),
        ),
        out_specs=(P("dp", None), P("dp"), P("dp")),
        check_vma=False,
    )
```

```python
import functools
import math
import jax
import jax.numpy as jnp
from jax import lax
from jax.experimental import pallas as pl
from jax.experimental.pallas import tpu as pltpu
from jax.sharding import PartitionSpec as P

SEQ_MB = 1

epsilon = 1e-05
ipo_tau = 0.5
MESH = pl.DeviceIdType.MESH
BATCHES = 4
PIECES = 4
ROUND = 2 * PIECES
HOP = 3
STEP = 4
ROOM = 59 * 1024 * 1024


def remote(src, dst, send_sem, recv_sem, target):
    return pltpu.make_async_remote_copy(
        src_ref=src,
        dst_ref=dst,
        send_sem=send_sem,
        recv_sem=recv_sem,
        device_id=target,
        device_id_type=MESH,
    )


def meet():
    barrier = pltpu.get_barrier_semaphore()
    n, count = lax.axis_size("dp"), lax.axis_size("mp")
    d, m, p = lax.axis_index("dp"), lax.axis_index("mp"), lax.axis_index("pipe")
    for k in range(1, n):
        pl.semaphore_signal(
            barrier, inc=1, device_id={"dp": lax.rem(d + k, n)}, device_id_type=MESH
        )
    for k in range(1, count):
        pl.semaphore_signal(
            barrier, inc=1, device_id={"mp": lax.rem(m + k, count)}, device_id_type=MESH
        )
    for k in range(count):
        pl.semaphore_signal(
            barrier,
            inc=1,
            device_id={"mp": lax.rem(m + k, count), "pipe": 1 - p},
            device_id_type=MESH,
        )
    pl.semaphore_wait(barrier, n - 1 + count - 1 + count)


def flat(ref):
    return jnp.concatenate([ref[s : s + 1, :] for s in range(ref.shape[0])], axis=1)


def per_sequence(row, seq_len):
    length = row.shape[1]
    lanes = lax.broadcasted_iota(jnp.int32, (length, 128), 1)
    spots = lax.broadcasted_iota(jnp.int32, (length, 128), 0)
    return lax.dot_general(
        jnp.broadcast_to(row, (8, length)),
        (lanes == spots // seq_len).astype(jnp.float32),
        (((1,), (0,)), ((), ())),
        precision=lax.Precision.HIGHEST,
        preferred_element_type=jnp.float32,
    )


def close_kernel(n, result_ref, mask_ref, anchor_ref, pairs_ref, token_ref, policy_ref, loss_ref):
    f32 = jnp.float32
    seq_count, seq_len = mask_ref.shape
    mask = flat(mask_ref).astype(f32)
    token = result_ref[:1, :]
    tallied = result_ref[1:2, :128]
    for s in range(seq_count):
        token_ref[s : s + 1, :] = token[:, s * seq_len : (s + 1) * seq_len]
    lane = lax.broadcasted_iota(jnp.int32, (8, 128), 1)
    divisor = jnp.where(lane < seq_count, tallied / (n * SEQ_MB), 1.0)
    policy = per_sequence(mask * token, seq_len) / divisor
    anchor = per_sequence(mask * flat(anchor_ref), seq_len) / divisor
    gaps = policy - anchor
    policy_ref[...] = policy[:1, :seq_count]
    losses = jnp.zeros((8, 128), f32)
    for i in range(seq_count // 2):
        chosen = jnp.sum(
            jnp.where(lane == pairs_ref[0, 2 * i], gaps, 0.0), axis=1, keepdims=True
        )
        rejected = jnp.sum(
            jnp.where(lane == pairs_ref[0, 2 * i + 1], gaps, 0.0), axis=1, keepdims=True
        )
        losses = jnp.where(lane == i, (chosen - rejected - 0.5 / ipo_tau) ** 2, losses)
    loss_ref[...] = losses[:1, : seq_count // 2]


def relay_kernel(
    x_hbm, up_hbm, down_hbm, head_hbm, layer_gain, final_gain, ids_ref, mask_ref,
    out_ref, full_ref, head, stats, tallies, up, down, xs, normed, xin, hid, act, ext, outs, rs, resid, nxt, slots, fin, scales,
    load, go, cs, cr, ns, nr, xs_s, xs_r, gs, gr, ins, inr, exr, bs, br, rss, rsr, ds, dr, qs, qr,
    hs, hr, fs, fr, es, er, load_head, ts, tr, vs, vr,
):
    n, count = lax.axis_size("dp"), lax.axis_size("mp")
    d, m, p = lax.axis_index("dp"), lax.axis_index("mp"), lax.axis_index("pipe")
    length, width = x_hbm.shape
    block, ff = up.shape
    part = length // count
    sub = part // BATCHES
    own_rows = sub * n
    batch = own_rows * count
    half = batch // 2
    piece = half // PIECES
    total = BATCHES * PIECES
    f32 = jnp.float32

    def rows(start, size):
        return pl.ds(pl.multiple_of(start, 16), size)

    def columns(owner):
        return pl.ds(pl.multiple_of(owner * block, 128), block)

    loads = [
        pltpu.make_async_copy(x_hbm.at[rows(m * part, part)], xs, load.at[0]),
        pltpu.make_async_copy(up_hbm, up, load.at[1]),
        pltpu.make_async_copy(down_hbm, down, load.at[2]),
    ]
    for copy in loads:
        copy.start()
    meet()
    seq_count, seq_len = mask_ref.shape

    mask = flat(mask_ref).astype(f32)
    tallies[0] = per_sequence(mask, seq_len)

    def tally(k):
        return remote(
            tallies.at[0], tallies.at[k], ts.at[k], tr.at[k], {"dp": lax.rem(d + k, n)}
        )

    loads[0].wait()

    def first_hop(b, k, owner):
        to = lax.rem(d + k, n)
        return remote(
            normed.at[rows(b * sub, sub), columns(to)],
            xin.at[rows(b * batch + (m * n + owner) * sub, sub)],
            ns.at[b, k],
            nr.at[b, k],
            {"dp": to},
        )

    def plain_hop(b, k, owner):
        to = lax.rem(d + k, n)
        return remote(
            xs.at[rows(b * sub, sub), columns(to)],
            resid.at[rows(b * own_rows + owner * sub, sub)],
            xs_s.at[b, k],
            xs_r.at[b, k],
            {"dp": to},
        )

    def share(b, k, owner):
        slab = xin.at[rows(b * batch + owner * own_rows, own_rows)]
        return remote(slab, slab, gs.at[b, k], gr.at[b, k], {"mp": lax.rem(m + k, count)})

    def pass_on(b, k, owner):
        return remote(
            nxt.at[rows(b * own_rows, own_rows)],
            xin.at[rows(b * batch + owner * own_rows, own_rows)],
            gs.at[b, k],
            gr.at[b, k],
            {"mp": lax.rem(m + k, count)},
        )

    def pass_scale(b, k, owner):
        slab = scales.at[rows(b * batch + owner * own_rows, own_rows)]
        return remote(slab, slab, cs.at[b, k], cr.at[b, k], {"mp": lax.rem(m + k, count)})

    def scatter(b, k):
        to = lax.rem(m + k, count)
        return remote(
            outs.at[rows(b * batch + to * own_rows, own_rows)],
            rs.at[rows((b * count + k) * own_rows, own_rows)],
            rss.at[b, k],
            rsr.at[b, k],
            {"mp": to, "pipe": 1 - p},
        )

    def hand_over(b):
        slab = rows(b * own_rows, own_rows)
        return remote(nxt.at[slab], resid.at[slab], ds.at[b], dr.at[b], {"pipe": 1 - p})

    def square(b, k):
        return remote(
            slots.at[b, 0], slots.at[b, k], qs.at[b, k], qr.at[b, k], {"dp": lax.rem(d + k, n)}
        )

    def last_hop(b, k, owner):
        to = lax.rem(d + k, n)
        return remote(
            nxt.at[rows(b * own_rows + to * sub, sub)],
            fin.at[b, owner],
            hs.at[b, k],
            hr.at[b, k],
            {"dp": to},
        )

    def spot(b, owner):
        return full_ref.at[rows(owner * part + b * sub, sub)]

    def full_share(b, k, owner):
        return remote(
            spot(b, owner), spot(b, owner), fs.at[b, k], fr.at[b, k], {"mp": lax.rem(m + k, count)}
        )

    def full_pass(b, k):
        owner = lax.rem(m - k + count, count)
        return remote(
            spot(b, owner), spot(b, owner), es.at[b, k], er.at[b, k], {"pipe": 1 - p}
        )

    def before(k):
        return lax.rem(d - k + n, n)

    def beside(k):
        return lax.rem(m - k + count, count)

    @pl.when(p == 0)
    def _():
        wide = xs[...].astype(f32)
        scale = lax.rsqrt(jnp.mean(wide * wide, axis=-1, keepdims=True) + epsilon)
        normed[...] = (wide * scale * layer_gain[...]).astype(normed.dtype)
        for b in range(BATCHES):
            for k in range(1, n):
                first_hop(b, k, d).start()
        for b in range(BATCHES):
            xin[rows(b * batch + (m * n + d) * sub, sub), :] = normed[
                b * sub : (b + 1) * sub, columns(d)
            ]
        for b in range(BATCHES):
            for k in range(1, n):
                first_hop(b, k, before(k)).wait_recv()
            for k in range(1, count):
                share(b, k, m).start()
        pl.semaphore_signal(go, inc=1, device_id={"pipe": 1 - p}, device_id_type=MESH)

    @pl.when(p == 1)
    def _():
        pl.semaphore_wait(go, 1)
        for b in range(BATCHES):
            for k in range(1, n):
                plain_hop(b, k, d).start()
            resid[rows(b * own_rows + d * sub, sub), :] = xs[b * sub : (b + 1) * sub, columns(d)]

    for k in range(1, n):
        tally(k).start()
    loads[1].wait()
    loads[2].wait()
    slots_head, tall, _ = head.shape
    vocab = head_hbm.shape[0]

    def head_load(j):
        return pltpu.make_async_copy(
            head_hbm.at[pl.ds(j * tall, tall)],
            head.at[j % slots_head],
            load_head.at[j % slots_head],
        )

    for j in range(slots_head):
        head_load(j).start()

    def enter(b):
        where = rows(b * batch, batch)

        @pl.when(p == 0)
        def _():
            for k in range(1, count):
                share(b, k, beside(k)).wait_recv()

        @pl.when(p == 1)
        def _():
            for k in range(1, count):
                pass_on(b, k, beside(k)).wait_recv()
                pass_scale(b, k, beside(k)).wait_recv()
            xin[where, :] = (
                xin[where, :].astype(f32) * scales[where, :1] * layer_gain[:, columns(d)]
            ).astype(xin.dtype)

        states = xin[where, :]
        hid[where, :] = jnp.dot(states, up[...], preferred_element_type=f32).astype(hid.dtype)

    def leave(b):
        where = rows(b * batch, batch)
        states = act[where, :]
        outs[where, :] = jnp.dot(states, down[...], preferred_element_type=f32).astype(outs.dtype)
        for k in (*range(1, count), 0):
            scatter(b, k).start()

    def add_up(b):
        for k in range(count):
            scatter(b, k).wait_recv()
        slab = rows(b * own_rows, own_rows)
        value = resid[slab, :].astype(f32)
        for k in range(count):
            value = value + rs[rows((b * count + k) * own_rows, own_rows), :].astype(f32)
        value = value.astype(nxt.dtype)
        nxt[slab, :] = value
        return value.astype(f32)

    def settle(b):
        for k in range(1, n):
            plain_hop(b, k, before(k)).wait_recv()
        wide = add_up(b)
        sums = jnp.sum(wide * wide, axis=1, keepdims=True)
        slots[b, 0] = jnp.broadcast_to(sums, (own_rows, 128))
        for k in range(1, n):
            square(b, k).start()
        for k in range(1, count):
            pass_on(b, k, m).start()
        hand_over(b).start()
        xin[rows(b * batch + m * own_rows, own_rows), :] = wide.astype(xin.dtype)

    def renew(b):
        sums = slots[b, 0]
        for k in range(1, n):
            square(b, k).wait_recv()
            sums = sums + slots[b, k]
        scales[rows(b * batch + m * own_rows, own_rows), :] = lax.rsqrt(sums / width + epsilon)
        for k in range(1, count):
            pass_scale(b, k, m).start()

    def span(way, c):
        b, k = lax.div(c, PIECES), lax.rem(c, PIECES)
        return rows(b * batch + way * half + k * piece, piece)

    def inner(way, c, to, into, sem):
        return remote(hid.at[span(way, c)], into, ins.at[way, c], sem.at[way, c], {"dp": to})

    def to_act(way, c, to):
        return inner(way, c, to, act.at[span(way, c)], inr)

    def to_ext(way, c, to):
        return inner(way, c, to, ext.at[rows(c * piece, piece)], exr)

    def outer(way, c, side):
        where = act.at[span(way, c)]
        to = d - 1 if side == 0 else d + 1
        return remote(where, where, bs.at[way, c, side], br.at[way, c], {"dp": to})

    offset = 2 * STEP + 1
    deep = HOP * (n // 2)
    ticks = offset + 2 * total + 2 * deep

    def tick(t, carry):
        now = t - offset
        for way in range(2):
            owner = n // 2 - way
            left, right = d < owner, d > owner
            hops = jnp.where(left, d, n - 1 - d)
            late = now - way - HOP * hops
            c = lax.div(late, 2)

            @pl.when((d != owner) & (late >= 0) & (lax.rem(late, 2) == 0) & (c < total))
            def _():
                here = span(way, c)

                @pl.when(hops > 0)
                def _():
                    to_act(way, c, d).wait_recv()
                    for j in range(0, ff, 256):
                        cut = slice(j, j + 256)
                        hid[here, cut] = (
                            hid[here, cut].astype(f32) + act[here, cut].astype(f32)
                        ).astype(hid.dtype)

                @pl.when(left)
                def _():
                    to_act(way, c, d + 1).start()

                @pl.when(right & (d - 1 > owner))
                def _():
                    to_act(way, c, d - 1).start()

                @pl.when(right & (d - 1 == owner))
                def _():
                    to_ext(way, c, d - 1).start()

        for way in range(2):
            owner = n // 2 - way
            late = now - way - deep
            c = lax.div(late, 2)

            @pl.when((d == owner) & (late >= 0) & (lax.rem(late, 2) == 0) & (c < total))
            def _():
                here = span(way, c)
                there = rows(c * piece, piece)
                if owner > 0:
                    to_act(way, c, d).wait_recv()
                if owner < n - 1:
                    to_ext(way, c, d).wait_recv()
                for j in range(0, ff, 256):
                    cut = slice(j, j + 256)
                    value = hid[here, cut].astype(f32)
                    if owner > 0:
                        value = value + act[here, cut].astype(f32)
                    if owner < n - 1:
                        value = value + ext[there, cut].astype(f32)
                    act[here, cut] = (value / (1.0 + jnp.exp(-value))).astype(act.dtype)
                if owner > 0:
                    outer(way, c, 0).start()
                if owner < n - 1:
                    outer(way, c, 1).start()

        for way in range(2):
            owner = n // 2 - way
            left, right = d < owner, d > owner
            away = jnp.where(left, owner - d, d - owner)
            late = now - way - deep - HOP * away
            c = lax.div(late, 2)

            @pl.when((d != owner) & (late >= 0) & (lax.rem(late, 2) == 0) & (c < total))
            def _():
                outer(way, c, 0).wait_recv()

                @pl.when(left & (d > 0))
                def _():
                    outer(way, c, 0).start()

                @pl.when(right & (d < n - 1))
                def _():
                    outer(way, c, 1).start()

        b = lax.div(now + 1, ROUND)

        @pl.when((now + 1 >= 0) & (lax.rem(now + 1, ROUND) == 0) & (b < BATCHES))
        def _():
            enter(b)

        done = now - (ROUND - 1) - 2 * deep
        q = lax.div(done, ROUND)

        @pl.when((done >= 0) & (lax.rem(done, ROUND) == 0) & (q < BATCHES))
        def _():
            leave(q)

        late = now + 1 + STEP
        e = lax.div(late, ROUND)

        @pl.when((p == 1) & (late >= 0) & (lax.rem(late, ROUND) == 0) & (e < BATCHES))
        def _():
            renew(e)

        early = now + 1 + 2 * STEP
        a = lax.div(early, ROUND)

        @pl.when((p == 1) & (lax.rem(early, ROUND) == 0) & (a < BATCHES))
        def _():
            settle(a)

        return carry

    lax.fori_loop(0, ticks, tick, 0)

    @pl.when(p == 0)
    def _():
        def finish(b, carry):
            hand_over(b).wait_recv()
            add_up(b)
            for k in range(1, n):
                last_hop(b, k, d).start()
            fin[b, d] = nxt[rows(b * own_rows + d * sub, sub), :]
            for k in range(1, n):
                last_hop(b, k, before(k)).wait_recv()
            sums = 0.0
            for g in range(n):
                wide = fin[b, g].astype(f32)
                sums = sums + jnp.sum(wide * wide, axis=1, keepdims=True)
            scale = lax.rsqrt(sums / width + epsilon)
            for g in range(n):
                cut = slice(g * block, (g + 1) * block)
                full_ref[rows(m * part + b * sub, sub), cut] = (
                    fin[b, g].astype(f32) * scale * final_gain[:, cut]
                ).astype(full_ref.dtype)
            for k in range(1, count):
                full_share(b, k, m).start()
            full_pass(b, 0).start()
            for k in range(1, count):
                full_share(b, k, beside(k)).wait_recv()
                full_pass(b, k).start()
            return carry

        lax.fori_loop(0, BATCHES, finish, 0)

    @pl.when(p == 1)
    def _():
        def finish(b, carry):
            for k in range(count):
                full_pass(b, k).wait_recv()
            return carry

        lax.fori_loop(0, BATCHES, finish, 0)

    states = full_ref[...]
    ids = flat(ids_ref) - (p * count + m) * vocab
    spots = lax.broadcasted_iota(jnp.int32, (tall, length), 0)
    top = jnp.full((1, length), -jnp.inf, f32)
    mass = jnp.zeros((1, length), f32)
    picked = jnp.zeros((1, length), f32)

    def gauge(j, logits, carry):
        top, mass, picked = carry
        peak = jnp.maximum(top, jnp.max(logits, axis=0, keepdims=True))
        mass = mass * jnp.exp(top - peak) + jnp.sum(jnp.exp(logits - peak), axis=0, keepdims=True)
        hit = jnp.where(spots == ids - j * tall, logits, 0.0)
        return peak, mass, picked + jnp.sum(hit, axis=0, keepdims=True)

    carry = top, mass, picked
    last = None
    for j in range(vocab // tall):
        head_load(j).wait()
        logits = jnp.concatenate(
            [
                lax.dot_general(
                    head[j % slots_head, cut : cut + tall // 2],
                    states,
                    (((1,), (1,)), ((), ())),
                    preferred_element_type=f32,
                )
                for cut in (0, tall // 2)
            ],
            axis=0,
        )
        if j + slots_head < vocab // tall:
            head_load(j + slots_head).start()
        if last is not None:
            carry = gauge(j - 1, last, carry)
        last = logits
    top, mass, picked = gauge(vocab // tall - 1, last, carry)

    def report(q, k):
        to = {"mp": lax.rem(m + k, count), "pipe": (p if q == 0 else 1 - p)}
        slot = q * count + k
        return remote(stats.at[0], stats.at[slot], vs.at[slot], vr.at[slot], to)

    others = [(q, k) for k in range(1, count) for q in range(2)] + [(1, 0)]
    stats[0] = jnp.concatenate([top, mass, picked, jnp.zeros((5, length), f32)], axis=0)
    for q, k in others:
        report(q, k).start()
    tallied = tallies[0]
    for k in range(1, n):
        tally(k).wait_recv()
        tallied = tallied + tallies[k]
    for q, k in others:
        report(q, k).wait_recv()
    peak = jnp.max(stats[:, 0, :], axis=0, keepdims=True)
    mass = jnp.sum(stats[:, 1, :] * jnp.exp(stats[:, 0, :] - peak), axis=0, keepdims=True)
    picked = jnp.sum(stats[:, 2, :], axis=0, keepdims=True)
    token = picked - peak - jnp.log(mass)
    out_ref[:1, :] = token
    out_ref[1:2, :128] = tallied[:1]
    for k in range(1, n):
        tally(k).wait_send()
    for q, k in others:
        report(q, k).wait_send()

    def drain(b, carry):
        for k in range(count):
            scatter(b, k).wait_send()

        @pl.when(p == 0)
        def _():
            for k in range(1, count):
                share(b, k, m).wait_send()
            for k in range(1, n):
                first_hop(b, k, d).wait_send()
                last_hop(b, k, d).wait_send()
            for k in range(1, count):
                full_share(b, k, m).wait_send()
            for k in range(count):
                full_pass(b, k).wait_send()

        @pl.when(p == 1)
        def _():
            for k in range(1, n):
                plain_hop(b, k, d).wait_send()
                square(b, k).wait_send()
            for k in range(1, count):
                pass_on(b, k, m).wait_send()
                pass_scale(b, k, m).wait_send()
            hand_over(b).wait_send()

        return carry

    lax.fori_loop(0, BATCHES, drain, 0)

    def drain_pieces(c, carry):
        for way in range(2):
            owner = n // 2 - way

            @pl.when(d != owner)
            def _():
                to_act(way, c, d).wait_send()

            @pl.when((d <= owner) & (d > 0))
            def _():
                outer(way, c, 0).wait_send()

            @pl.when((d >= owner) & (d < n - 1))
            def _():
                outer(way, c, 1).wait_send()

        return carry

    lax.fori_loop(0, total, drain_pieces, 0)


def sems(*shape):
    return [pltpu.SemaphoreType.DMA(shape)] * 2


def shards(
    hidden_states,
    up_weight,
    down_weight,
    layer_gain,
    final_gain,
    unembedding,
    target_ids,
    response_masks,
    anchor_logps,
    pairing,
):
    seq_count, length, model_width = hidden_states.shape
    groups = lax.axis_size("dp")
    vp_size = lax.axis_size("pipe") * lax.axis_size("mp")
    rows = seq_count * length
    block = model_width // groups
    ff = up_weight.shape[2]
    count = lax.axis_size("mp")
    bf16 = jnp.bfloat16
    part = rows // count
    own_rows = part * groups
    all_rows = rows * groups
    steps = BATCHES * PIECES
    vocab = unembedding.shape[0]
    anyspec = pl.BlockSpec(memory_space=pl.ANY)
    spec = pl.BlockSpec(memory_space=pltpu.VMEM)
    smem = pl.BlockSpec(memory_space=pltpu.SMEM)
    dma = pltpu.SemaphoreType.DMA
    buffers = [
        ((rows, model_width), bf16),
        None,
        ((vp_size, 8, rows), jnp.float32),
        ((groups, 8, 128), jnp.float32),
        ((block, ff), bf16),
        ((ff, block), bf16),
        ((part, model_width), bf16),
        ((part, model_width), bf16),
        ((all_rows, block), bf16),
        ((all_rows, ff), bf16),
        ((all_rows, ff), bf16),
        ((all_rows // 2, ff), bf16),
        ((all_rows, block), bf16),
        ((all_rows, block), bf16),
        ((own_rows, block), bf16),
        ((own_rows, block), bf16),
        ((BATCHES, groups, own_rows // BATCHES, 128), jnp.float32),
        ((BATCHES, groups, part // BATCHES, block), bf16),
        ((all_rows, 128), jnp.float32),
    ]
    used = sum(math.prod(b[0]) * jnp.dtype(b[1]).itemsize for b in buffers if b)
    cuts = 8
    while used + vocab // cuts * model_width * 2 > ROOM:
        cuts *= 2
    tall = vocab // cuts
    kept = min(cuts, (ROOM - used) // (tall * model_width * 2))
    buffers[1] = ((kept, tall, model_width), bf16)
    result = pl.pallas_call(
        relay_kernel,
        name="relay",
        out_shape=jax.ShapeDtypeStruct((2, rows), jnp.float32),
        in_specs=[anyspec] * 4 + [spec] * 4,
        out_specs=spec,
        scratch_shapes=[pltpu.VMEM(*b) for b in buffers]
        + [dma((3,)), pltpu.SemaphoreType.REGULAR]
        + sems(BATCHES, count)
        + sems(BATCHES, groups)
        + sems(BATCHES, groups)
        + sems(BATCHES, count)
        + [dma((2, steps))] * 3
        + [dma((2, steps, 2)), dma((2, steps))]
        + sems(BATCHES, count)
        + sems(BATCHES)
        + sems(BATCHES, groups)
        + sems(BATCHES, groups)
        + sems(BATCHES, count)
        + sems(BATCHES, count)
        + [dma((kept,))]
        + sems(groups)
        + sems(vp_size),
        compiler_params=pltpu.CompilerParams(
            collective_id=0, has_side_effects=True, vmem_limit_bytes=67043328
        ),
    )(
        hidden_states.reshape(rows, model_width),
        up_weight[0],
        down_weight[0],
        unembedding,
        layer_gain,
        final_gain[None],
        target_ids,
        response_masks,
    )
    token_logps, policy, losses = pl.pallas_call(
        functools.partial(close_kernel, groups),
        name="close",
        out_shape=[
            jax.ShapeDtypeStruct(target_ids.shape, jnp.float32),
            jax.ShapeDtypeStruct((1, seq_count), jnp.float32),
            jax.ShapeDtypeStruct((1, seq_count // 2), jnp.float32),
        ],
        in_specs=[spec] * 3 + [smem],
        out_specs=[spec] * 3,
    )(result, response_masks, anchor_logps, pairing)
    return token_logps, policy[0], losses[0]


def solution(mesh):
    return jax.shard_map(
        shards,
        mesh=mesh,
        in_specs=(
            P("dp", None, None),
            P("pipe", "dp", "mp"),
            P("pipe", "mp", "dp"),
            P("pipe", None),
            P(),
            P(("pipe", "mp"), None),
            P("dp", None),
            P("dp", None),
            P("dp", None),
            P("dp", None),
        ),
        out_specs=(P("dp", None), P("dp"), P("dp")),
        check_vma=False,
    )
```

```python
import functools
import math
import jax
import jax.numpy as jnp
from jax import lax
from jax.experimental import pallas as pl
from jax.experimental.pallas import tpu as pltpu
from jax.sharding import PartitionSpec as P

SEQ_MB = 1

epsilon = 1e-05
ipo_tau = 0.5
MESH = pl.DeviceIdType.MESH
BATCHES = 4
PIECES = 4
ROUND = 2 * PIECES
HOP = 3
STEP = 4
ROOM = 59 * 1024 * 1024


def remote(src, dst, send_sem, recv_sem, target):
    return pltpu.make_async_remote_copy(
        src_ref=src,
        dst_ref=dst,
        send_sem=send_sem,
        recv_sem=recv_sem,
        device_id=target,
        device_id_type=MESH,
    )


def meet():
    barrier = pltpu.get_barrier_semaphore()
    n, count = lax.axis_size("dp"), lax.axis_size("mp")
    d, m, p = lax.axis_index("dp"), lax.axis_index("mp"), lax.axis_index("pipe")
    for k in range(1, n):
        pl.semaphore_signal(
            barrier, inc=1, device_id={"dp": lax.rem(d + k, n)}, device_id_type=MESH
        )
    for k in range(1, count):
        pl.semaphore_signal(
            barrier, inc=1, device_id={"mp": lax.rem(m + k, count)}, device_id_type=MESH
        )
    for k in range(count):
        pl.semaphore_signal(
            barrier,
            inc=1,
            device_id={"mp": lax.rem(m + k, count), "pipe": 1 - p},
            device_id_type=MESH,
        )
    pl.semaphore_wait(barrier, n - 1 + count - 1 + count)


def flat(ref):
    return jnp.concatenate([ref[s : s + 1, :] for s in range(ref.shape[0])], axis=1)


def per_sequence(row, seq_len):
    length = row.shape[1]
    lanes = lax.broadcasted_iota(jnp.int32, (length, 128), 1)
    spots = lax.broadcasted_iota(jnp.int32, (length, 128), 0)
    return lax.dot_general(
        jnp.broadcast_to(row, (8, length)),
        (lanes == spots // seq_len).astype(jnp.float32),
        (((1,), (0,)), ((), ())),
        precision=lax.Precision.HIGHEST,
        preferred_element_type=jnp.float32,
    )


def close_kernel(n, result_ref, mask_ref, anchor_ref, pairs_ref, token_ref, policy_ref, loss_ref):
    f32 = jnp.float32
    seq_count, seq_len = mask_ref.shape
    mask = flat(mask_ref).astype(f32)
    token = result_ref[:1, :]
    tallied = result_ref[1:2, :128]
    for s in range(seq_count):
        token_ref[s : s + 1, :] = token[:, s * seq_len : (s + 1) * seq_len]
    lane = lax.broadcasted_iota(jnp.int32, (8, 128), 1)
    divisor = jnp.where(lane < seq_count, tallied / (n * SEQ_MB), 1.0)
    policy = per_sequence(mask * token, seq_len) / divisor
    anchor = per_sequence(mask * flat(anchor_ref), seq_len) / divisor
    gaps = policy - anchor
    policy_ref[...] = policy[:1, :seq_count]
    losses = jnp.zeros((8, 128), f32)
    for i in range(seq_count // 2):
        chosen = jnp.sum(
            jnp.where(lane == pairs_ref[0, 2 * i], gaps, 0.0), axis=1, keepdims=True
        )
        rejected = jnp.sum(
            jnp.where(lane == pairs_ref[0, 2 * i + 1], gaps, 0.0), axis=1, keepdims=True
        )
        losses = jnp.where(lane == i, (chosen - rejected - 0.5 / ipo_tau) ** 2, losses)
    loss_ref[...] = losses[:1, : seq_count // 2]


def relay_kernel(
    x_hbm, up_hbm, down_hbm, head_hbm, layer_gain, final_gain, ids_ref, mask_ref,
    out_ref, full_ref, head, stats, tallies, up, down, xs, normed, xin, hid, act, ext, outs, rs, resid, nxt, slots, fin, scales,
    load, go, cs, cr, ns, nr, xs_s, xs_r, gs, gr, ins, inr, exr, bs, br, rss, rsr, ds, dr, qs, qr,
    hs, hr, fs, fr, es, er, load_head, ts, tr, vs, vr,
):
    n, count = lax.axis_size("dp"), lax.axis_size("mp")
    d, m, p = lax.axis_index("dp"), lax.axis_index("mp"), lax.axis_index("pipe")
    length, width = x_hbm.shape
    block, ff = up.shape
    part = length // count
    sub = part // BATCHES
    own_rows = sub * n
    batch = own_rows * count
    half = batch // 2
    piece = half // PIECES
    total = BATCHES * PIECES
    f32 = jnp.float32

    def rows(start, size):
        return pl.ds(pl.multiple_of(start, 16), size)

    def columns(owner):
        return pl.ds(pl.multiple_of(owner * block, 128), block)

    loads = [
        pltpu.make_async_copy(x_hbm.at[rows(m * part, part)], xs, load.at[0]),
        pltpu.make_async_copy(up_hbm, up, load.at[1]),
        pltpu.make_async_copy(down_hbm, down, load.at[2]),
    ]
    for copy in loads:
        copy.start()
    meet()
    seq_count, seq_len = mask_ref.shape

    mask = flat(mask_ref).astype(f32)
    tallies[0] = per_sequence(mask, seq_len)

    def tally(k):
        return remote(
            tallies.at[0], tallies.at[k], ts.at[k], tr.at[k], {"dp": lax.rem(d + k, n)}
        )

    loads[0].wait()

    def first_hop(b, k, owner):
        to = lax.rem(d + k, n)
        return remote(
            normed.at[rows(b * sub, sub), columns(to)],
            xin.at[rows(b * batch + (m * n + owner) * sub, sub)],
            ns.at[b, k],
            nr.at[b, k],
            {"dp": to},
        )

    def plain_hop(b, k, owner):
        to = lax.rem(d + k, n)
        return remote(
            xs.at[rows(b * sub, sub), columns(to)],
            resid.at[rows(b * own_rows + owner * sub, sub)],
            xs_s.at[b, k],
            xs_r.at[b, k],
            {"dp": to},
        )

    def share(b, k, owner):
        slab = xin.at[rows(b * batch + owner * own_rows, own_rows)]
        return remote(slab, slab, gs.at[b, k], gr.at[b, k], {"mp": lax.rem(m + k, count)})

    def pass_on(b, k, owner):
        return remote(
            nxt.at[rows(b * own_rows, own_rows)],
            xin.at[rows(b * batch + owner * own_rows, own_rows)],
            gs.at[b, k],
            gr.at[b, k],
            {"mp": lax.rem(m + k, count)},
        )

    def pass_scale(b, k, owner):
        slab = scales.at[rows(b * batch + owner * own_rows, own_rows)]
        return remote(slab, slab, cs.at[b, k], cr.at[b, k], {"mp": lax.rem(m + k, count)})

    def scatter(b, k):
        to = lax.rem(m + k, count)
        return remote(
            outs.at[rows(b * batch + to * own_rows, own_rows)],
            rs.at[rows((b * count + k) * own_rows, own_rows)],
            rss.at[b, k],
            rsr.at[b, k],
            {"mp": to, "pipe": 1 - p},
        )

    def hand_over(b):
        slab = rows(b * own_rows, own_rows)
        return remote(nxt.at[slab], resid.at[slab], ds.at[b], dr.at[b], {"pipe": 1 - p})

    def square(b, k):
        return remote(
            slots.at[b, 0], slots.at[b, k], qs.at[b, k], qr.at[b, k], {"dp": lax.rem(d + k, n)}
        )

    def last_hop(b, k, owner):
        to = lax.rem(d + k, n)
        return remote(
            nxt.at[rows(b * own_rows + to * sub, sub)],
            fin.at[b, owner],
            hs.at[b, k],
            hr.at[b, k],
            {"dp": to},
        )

    def spot(b, owner):
        return full_ref.at[rows(owner * part + b * sub, sub)]

    def full_share(b, k, owner):
        return remote(
            spot(b, owner), spot(b, owner), fs.at[b, k], fr.at[b, k], {"mp": lax.rem(m + k, count)}
        )

    def full_pass(b, k):
        owner = lax.rem(m - k + count, count)
        return remote(
            spot(b, owner), spot(b, owner), es.at[b, k], er.at[b, k], {"pipe": 1 - p}
        )

    def before(k):
        return lax.rem(d - k + n, n)

    def beside(k):
        return lax.rem(m - k + count, count)

    @pl.when(p == 0)
    def _():
        for b in range(BATCHES):
            cut = slice(b * sub, (b + 1) * sub)
            wide = xs[cut, :].astype(f32)
            scale = lax.rsqrt(jnp.mean(wide * wide, axis=-1, keepdims=True) + epsilon)
            normed[cut, :] = (wide * scale * layer_gain[...]).astype(normed.dtype)
            for k in range(1, n):
                first_hop(b, k, d).start()
        for b in range(BATCHES):
            xin[rows(b * batch + (m * n + d) * sub, sub), :] = normed[
                b * sub : (b + 1) * sub, columns(d)
            ]
        for b in range(BATCHES):
            for k in range(1, n):
                first_hop(b, k, before(k)).wait_recv()
            for k in range(1, count):
                share(b, k, m).start()
        pl.semaphore_signal(go, inc=1, device_id={"pipe": 1 - p}, device_id_type=MESH)

    @pl.when(p == 1)
    def _():
        pl.semaphore_wait(go, 1)
        for b in range(BATCHES):
            for k in range(1, n):
                plain_hop(b, k, d).start()
            resid[rows(b * own_rows + d * sub, sub), :] = xs[b * sub : (b + 1) * sub, columns(d)]

    for k in range(1, n):
        tally(k).start()
    loads[1].wait()
    loads[2].wait()
    slots_head, tall, _ = head.shape
    vocab = head_hbm.shape[0]

    def head_load(j):
        return pltpu.make_async_copy(
            head_hbm.at[pl.ds(j * tall, tall)],
            head.at[j % slots_head],
            load_head.at[j % slots_head],
        )

    for j in range(slots_head):
        head_load(j).start()

    def enter(b):
        where = rows(b * batch, batch)

        @pl.when(p == 0)
        def _():
            for k in range(1, count):
                share(b, k, beside(k)).wait_recv()

        @pl.when(p == 1)
        def _():
            for k in range(1, count):
                pass_on(b, k, beside(k)).wait_recv()
                pass_scale(b, k, beside(k)).wait_recv()
            xin[where, :] = (
                xin[where, :].astype(f32) * scales[where, :1] * layer_gain[:, columns(d)]
            ).astype(xin.dtype)

        states = xin[where, :]
        hid[where, :] = jnp.dot(states, up[...], preferred_element_type=f32).astype(hid.dtype)

    def leave(b):
        where = rows(b * batch, batch)
        states = act[where, :]
        outs[where, :] = jnp.dot(states, down[...], preferred_element_type=f32).astype(outs.dtype)
        for k in (*range(1, count), 0):
            scatter(b, k).start()

    def add_up(b):
        for k in range(count):
            scatter(b, k).wait_recv()
        slab = rows(b * own_rows, own_rows)
        value = resid[slab, :].astype(f32)
        for k in range(count):
            value = value + rs[rows((b * count + k) * own_rows, own_rows), :].astype(f32)
        value = value.astype(nxt.dtype)
        nxt[slab, :] = value
        return value.astype(f32)

    def settle(b):
        for k in range(1, n):
            plain_hop(b, k, before(k)).wait_recv()
        wide = add_up(b)
        sums = jnp.sum(wide * wide, axis=1, keepdims=True)
        slots[b, 0] = jnp.broadcast_to(sums, (own_rows, 128))
        for k in range(1, n):
            square(b, k).start()
        for k in range(1, count):
            pass_on(b, k, m).start()
        hand_over(b).start()
        xin[rows(b * batch + m * own_rows, own_rows), :] = wide.astype(xin.dtype)

    def renew(b):
        sums = slots[b, 0]
        for k in range(1, n):
            square(b, k).wait_recv()
            sums = sums + slots[b, k]
        scales[rows(b * batch + m * own_rows, own_rows), :] = lax.rsqrt(sums / width + epsilon)
        for k in range(1, count):
            pass_scale(b, k, m).start()

    def span(way, c):
        b, k = lax.div(c, PIECES), lax.rem(c, PIECES)
        return rows(b * batch + way * half + k * piece, piece)

    def inner(way, c, to, into, sem):
        return remote(hid.at[span(way, c)], into, ins.at[way, c], sem.at[way, c], {"dp": to})

    def to_act(way, c, to):
        return inner(way, c, to, act.at[span(way, c)], inr)

    def to_ext(way, c, to):
        return inner(way, c, to, ext.at[rows(c * piece, piece)], exr)

    def outer(way, c, side):
        where = act.at[span(way, c)]
        to = d - 1 if side == 0 else d + 1
        return remote(where, where, bs.at[way, c, side], br.at[way, c], {"dp": to})

    offset = 2 * STEP + 1
    deep = HOP * (n // 2)
    ticks = offset + 2 * total + 2 * deep

    def tick(t, carry):
        now = t - offset
        for way in range(2):
            owner = n // 2 - way
            left, right = d < owner, d > owner
            hops = jnp.where(left, d, n - 1 - d)
            late = now - way - HOP * hops
            c = lax.div(late, 2)

            @pl.when((d != owner) & (late >= 0) & (lax.rem(late, 2) == 0) & (c < total))
            def _():
                here = span(way, c)

                @pl.when(hops > 0)
                def _():
                    to_act(way, c, d).wait_recv()
                    for j in range(0, ff, 256):
                        cut = slice(j, j + 256)
                        hid[here, cut] = (
                            hid[here, cut].astype(f32) + act[here, cut].astype(f32)
                        ).astype(hid.dtype)

                @pl.when(left)
                def _():
                    to_act(way, c, d + 1).start()

                @pl.when(right & (d - 1 > owner))
                def _():
                    to_act(way, c, d - 1).start()

                @pl.when(right & (d - 1 == owner))
                def _():
                    to_ext(way, c, d - 1).start()

        for way in range(2):
            owner = n // 2 - way
            late = now - way - deep
            c = lax.div(late, 2)

            @pl.when((d == owner) & (late >= 0) & (lax.rem(late, 2) == 0) & (c < total))
            def _():
                here = span(way, c)
                there = rows(c * piece, piece)
                if owner > 0:
                    to_act(way, c, d).wait_recv()
                if owner < n - 1:
                    to_ext(way, c, d).wait_recv()
                for j in range(0, ff, 256):
                    cut = slice(j, j + 256)
                    value = hid[here, cut].astype(f32)
                    if owner > 0:
                        value = value + act[here, cut].astype(f32)
                    if owner < n - 1:
                        value = value + ext[there, cut].astype(f32)
                    act[here, cut] = (value / (1.0 + jnp.exp(-value))).astype(act.dtype)
                if owner > 0:
                    outer(way, c, 0).start()
                if owner < n - 1:
                    outer(way, c, 1).start()

        for way in range(2):
            owner = n // 2 - way
            left, right = d < owner, d > owner
            away = jnp.where(left, owner - d, d - owner)
            late = now - way - deep - HOP * away
            c = lax.div(late, 2)

            @pl.when((d != owner) & (late >= 0) & (lax.rem(late, 2) == 0) & (c < total))
            def _():
                outer(way, c, 0).wait_recv()

                @pl.when(left & (d > 0))
                def _():
                    outer(way, c, 0).start()

                @pl.when(right & (d < n - 1))
                def _():
                    outer(way, c, 1).start()

        b = lax.div(now + 1, ROUND)

        @pl.when((now + 1 >= 0) & (lax.rem(now + 1, ROUND) == 0) & (b < BATCHES))
        def _():
            enter(b)

        done = now - (ROUND - 1) - 2 * deep
        q = lax.div(done, ROUND)

        @pl.when((done >= 0) & (lax.rem(done, ROUND) == 0) & (q < BATCHES))
        def _():
            leave(q)

        late = now + 1 + STEP
        e = lax.div(late, ROUND)

        @pl.when((p == 1) & (late >= 0) & (lax.rem(late, ROUND) == 0) & (e < BATCHES))
        def _():
            renew(e)

        early = now + 1 + 2 * STEP
        a = lax.div(early, ROUND)

        @pl.when((p == 1) & (lax.rem(early, ROUND) == 0) & (a < BATCHES))
        def _():
            settle(a)

        return carry

    lax.fori_loop(0, ticks, tick, 0)

    @pl.when(p == 0)
    def _():
        def finish(b, carry):
            hand_over(b).wait_recv()
            add_up(b)
            for k in range(1, n):
                last_hop(b, k, d).start()
            fin[b, d] = nxt[rows(b * own_rows + d * sub, sub), :]
            for k in range(1, n):
                last_hop(b, k, before(k)).wait_recv()
            sums = 0.0
            for g in range(n):
                wide = fin[b, g].astype(f32)
                sums = sums + jnp.sum(wide * wide, axis=1, keepdims=True)
            scale = lax.rsqrt(sums / width + epsilon)
            for g in range(n):
                cut = slice(g * block, (g + 1) * block)
                full_ref[rows(m * part + b * sub, sub), cut] = (
                    fin[b, g].astype(f32) * scale * final_gain[:, cut]
                ).astype(full_ref.dtype)
            for k in range(1, count):
                full_share(b, k, m).start()
            full_pass(b, 0).start()
            for k in range(1, count):
                full_share(b, k, beside(k)).wait_recv()
                full_pass(b, k).start()
            return carry

        lax.fori_loop(0, BATCHES, finish, 0)

    @pl.when(p == 1)
    def _():
        def finish(b, carry):
            for k in range(count):
                full_pass(b, k).wait_recv()
            return carry

        lax.fori_loop(0, BATCHES, finish, 0)

    states = full_ref[...]
    ids = flat(ids_ref) - (p * count + m) * vocab
    spots = lax.broadcasted_iota(jnp.int32, (tall, length), 0)
    top = jnp.full((1, length), -jnp.inf, f32)
    mass = jnp.zeros((1, length), f32)
    picked = jnp.zeros((1, length), f32)

    def gauge(j, logits, carry):
        top, mass, picked = carry
        peak = jnp.maximum(top, jnp.max(logits, axis=0, keepdims=True))
        mass = mass * jnp.exp(top - peak) + jnp.sum(jnp.exp(logits - peak), axis=0, keepdims=True)
        hit = jnp.where(spots == ids - j * tall, logits, 0.0)
        return peak, mass, picked + jnp.sum(hit, axis=0, keepdims=True)

    carry = top, mass, picked
    last = None
    for j in range(vocab // tall):
        head_load(j).wait()
        logits = jnp.concatenate(
            [
                lax.dot_general(
                    head[j % slots_head, cut : cut + tall // 2],
                    states,
                    (((1,), (1,)), ((), ())),
                    preferred_element_type=f32,
                )
                for cut in (0, tall // 2)
            ],
            axis=0,
        )
        if j + slots_head < vocab // tall:
            head_load(j + slots_head).start()
        if last is not None:
            carry = gauge(j - 1, last, carry)
        last = logits
    top, mass, picked = gauge(vocab // tall - 1, last, carry)

    def report(q, k):
        to = {"mp": lax.rem(m + k, count), "pipe": (p if q == 0 else 1 - p)}
        slot = q * count + k
        return remote(stats.at[0], stats.at[slot], vs.at[slot], vr.at[slot], to)

    others = [(q, k) for k in range(1, count) for q in range(2)] + [(1, 0)]
    stats[0] = jnp.concatenate([top, mass, picked, jnp.zeros((5, length), f32)], axis=0)
    for q, k in others:
        report(q, k).start()
    tallied = tallies[0]
    for k in range(1, n):
        tally(k).wait_recv()
        tallied = tallied + tallies[k]
    for q, k in others:
        report(q, k).wait_recv()
    peak = jnp.max(stats[:, 0, :], axis=0, keepdims=True)
    mass = jnp.sum(stats[:, 1, :] * jnp.exp(stats[:, 0, :] - peak), axis=0, keepdims=True)
    picked = jnp.sum(stats[:, 2, :], axis=0, keepdims=True)
    token = picked - peak - jnp.log(mass)
    out_ref[:1, :] = token
    out_ref[1:2, :128] = tallied[:1]
    for k in range(1, n):
        tally(k).wait_send()
    for q, k in others:
        report(q, k).wait_send()

    def drain(b, carry):
        for k in range(count):
            scatter(b, k).wait_send()

        @pl.when(p == 0)
        def _():
            for k in range(1, count):
                share(b, k, m).wait_send()
            for k in range(1, n):
                first_hop(b, k, d).wait_send()
                last_hop(b, k, d).wait_send()
            for k in range(1, count):
                full_share(b, k, m).wait_send()
            for k in range(count):
                full_pass(b, k).wait_send()

        @pl.when(p == 1)
        def _():
            for k in range(1, n):
                plain_hop(b, k, d).wait_send()
                square(b, k).wait_send()
            for k in range(1, count):
                pass_on(b, k, m).wait_send()
                pass_scale(b, k, m).wait_send()
            hand_over(b).wait_send()

        return carry

    lax.fori_loop(0, BATCHES, drain, 0)

    def drain_pieces(c, carry):
        for way in range(2):
            owner = n // 2 - way

            @pl.when(d != owner)
            def _():
                to_act(way, c, d).wait_send()

            @pl.when((d <= owner) & (d > 0))
            def _():
                outer(way, c, 0).wait_send()

            @pl.when((d >= owner) & (d < n - 1))
            def _():
                outer(way, c, 1).wait_send()

        return carry

    lax.fori_loop(0, total, drain_pieces, 0)


def sems(*shape):
    return [pltpu.SemaphoreType.DMA(shape)] * 2


def shards(
    hidden_states,
    up_weight,
    down_weight,
    layer_gain,
    final_gain,
    unembedding,
    target_ids,
    response_masks,
    anchor_logps,
    pairing,
):
    seq_count, length, model_width = hidden_states.shape
    groups = lax.axis_size("dp")
    vp_size = lax.axis_size("pipe") * lax.axis_size("mp")
    rows = seq_count * length
    block = model_width // groups
    ff = up_weight.shape[2]
    count = lax.axis_size("mp")
    bf16 = jnp.bfloat16
    part = rows // count
    own_rows = part * groups
    all_rows = rows * groups
    steps = BATCHES * PIECES
    vocab = unembedding.shape[0]
    anyspec = pl.BlockSpec(memory_space=pl.ANY)
    spec = pl.BlockSpec(memory_space=pltpu.VMEM)
    smem = pl.BlockSpec(memory_space=pltpu.SMEM)
    dma = pltpu.SemaphoreType.DMA
    buffers = [
        ((rows, model_width), bf16),
        None,
        ((vp_size, 8, rows), jnp.float32),
        ((groups, 8, 128), jnp.float32),
        ((block, ff), bf16),
        ((ff, block), bf16),
        ((part, model_width), bf16),
        ((part, model_width), bf16),
        ((all_rows, block), bf16),
        ((all_rows, ff), bf16),
        ((all_rows, ff), bf16),
        ((all_rows // 2, ff), bf16),
        ((all_rows, block), bf16),
        ((all_rows, block), bf16),
        ((own_rows, block), bf16),
        ((own_rows, block), bf16),
        ((BATCHES, groups, own_rows // BATCHES, 128), jnp.float32),
        ((BATCHES, groups, part // BATCHES, block), bf16),
        ((all_rows, 128), jnp.float32),
    ]
    used = sum(math.prod(b[0]) * jnp.dtype(b[1]).itemsize for b in buffers if b)
    cuts = 8
    while used + vocab // cuts * model_width * 2 > ROOM:
        cuts *= 2
    tall = vocab // cuts
    kept = min(cuts, (ROOM - used) // (tall * model_width * 2))
    buffers[1] = ((kept, tall, model_width), bf16)
    result = pl.pallas_call(
        relay_kernel,
        name="relay",
        out_shape=jax.ShapeDtypeStruct((2, rows), jnp.float32),
        in_specs=[anyspec] * 4 + [spec] * 4,
        out_specs=spec,
        scratch_shapes=[pltpu.VMEM(*b) for b in buffers]
        + [dma((3,)), pltpu.SemaphoreType.REGULAR]
        + sems(BATCHES, count)
        + sems(BATCHES, groups)
        + sems(BATCHES, groups)
        + sems(BATCHES, count)
        + [dma((2, steps))] * 3
        + [dma((2, steps, 2)), dma((2, steps))]
        + sems(BATCHES, count)
        + sems(BATCHES)
        + sems(BATCHES, groups)
        + sems(BATCHES, groups)
        + sems(BATCHES, count)
        + sems(BATCHES, count)
        + [dma((kept,))]
        + sems(groups)
        + sems(vp_size),
        compiler_params=pltpu.CompilerParams(
            collective_id=0, has_side_effects=True, vmem_limit_bytes=67043328
        ),
    )(
        hidden_states.reshape(rows, model_width),
        up_weight[0],
        down_weight[0],
        unembedding,
        layer_gain,
        final_gain[None],
        target_ids,
        response_masks,
    )
    token_logps, policy, losses = pl.pallas_call(
        functools.partial(close_kernel, groups),
        name="close",
        out_shape=[
            jax.ShapeDtypeStruct(target_ids.shape, jnp.float32),
            jax.ShapeDtypeStruct((1, seq_count), jnp.float32),
            jax.ShapeDtypeStruct((1, seq_count // 2), jnp.float32),
        ],
        in_specs=[spec] * 3 + [smem],
        out_specs=[spec] * 3,
    )(result, response_masks, anchor_logps, pairing)
    return token_logps, policy[0], losses[0]


def solution(mesh):
    return jax.shard_map(
        shards,
        mesh=mesh,
        in_specs=(
            P("dp", None, None),
            P("pipe", "dp", "mp"),
            P("pipe", "mp", "dp"),
            P("pipe", None),
            P(),
            P(("pipe", "mp"), None),
            P("dp", None),
            P("dp", None),
            P("dp", None),
            P("dp", None),
        ),
        out_specs=(P("dp", None), P("dp"), P("dp")),
        check_vma=False,
    )
```
